32 devices in a mesh: side: 8 (over y, x, core), lane: 4 (over z).
Axes of the slice: x: 2, y: 2, z: 4, core: 2. Of those that a mesh axis runs over, the one named last changes fastest.
Arguments:
- tokens: bfloat16 [4096, 2048], P(('side', 'lane')), may hold values from -6 to 6
- expert_ids: int32 [4096, 8], P(('side', 'lane')), may hold values from 0 to 31, all different within a row; in each aligned block of 128 rows (0 to 127, 128 to 255, ...) at most 64 rows name the same one
- route_weights: float32 [4096, 8], P(('side', 'lane')), may hold values from 0.03 to 0.4
- w_gate: bfloat16 [32, 2048, 768], P(('side', 'lane')), may hold values from -0.125 to 0.125
- w_up: bfloat16 [32, 2048, 768], P(('side', 'lane')), may hold values from -0.125 to 0.125
- w_down: bfloat16 [32, 768, 2048], P(('side', 'lane')), may hold values from -0.21875 to 0.21875
Outputs:
- mixed: bfloat16 [4096, 2048], P(('side', 'lane'))
The draws below stay inside these ranges and needn't reach their ends.
Inputs may be any that keep to these rules, and one draw needn't show every extreme that they name: `expert_ids`: each row names 8 different experts. Within each aligned block of 128 rows (the rows of one device) no expert is named by more than 64 rows, and in every draw some expert is named by exactly 64 rows of some block.
All inputs are finite; a program needn't handle non-finite values.
Results may differ from the reference program's by a relative error of at most 0.0085.
Values may be sent and summed in bfloat16 or wider, within the bound.
A program may use at most 128 MiB of HBM per device.

```python
import math
import jax
import jax.numpy as jnp
import numpy as np
from jax import lax

D = 2048
FFE = 768
TOP = 8
TOK_DEV = 128
EXPERTS = 32
TOKENS = 4096
CAP = 64


def steps_of(rng, dims, cuts, smallest, top_value):
    def one(position, shards_of):
        heights = jax.random.uniform(jax.random.fold_in(jax.random.fold_in(rng, 6), position), (shards_of,), jnp.float32, smallest / len(cuts), top_value / len(cuts))
        return jnp.repeat(jnp.exp(heights), dims[position] // shards_of).reshape((-1,) + (1,) * (len(dims) - position - 1))

    level = one(*cuts[0])
    for cut in cuts[1:]:
        level = level * one(*cut)
    return level


def routed_block(key, own, number, rows, amount, top, bound, lean):
    sequence = jax.random.permutation(key, amount)
    packed, usual = shares(amount, rows * top, bound, lean, True), shares(amount, rows * top, bound, lean, False)
    places = jnp.arange(amount)

    def named(tallies, offset_by):
        used = int((tallies > 0).sum())
        fixed = max(1, used // 4)
        passed = fixed + (places - fixed + offset_by * (used - fixed)) % max(1, amount - fixed)
        return jnp.zeros((amount,), jnp.int32).at[sequence[jnp.where(places < fixed, places, passed)]].set(jnp.asarray(tallies, jnp.int32))

    tallies = jnp.where(number % 4 == 0, named(packed, number // 4), named(usual, number - number // 4 - 1))
    mixed = jax.random.permutation(jax.random.fold_in(own, 3), amount)
    donor, taker = mixed[0:amount // 2 * 2:2], mixed[1:amount // 2 * 2:2]
    room = jnp.minimum(tallies[donor] - 1, bound - tallies[taker]) // 2
    room = jnp.where((donor == sequence[0]) | (taker == sequence[0]) | (tallies[taker] == 0), 0, jnp.maximum(room, 0))
    passed = jax.random.randint(jax.random.fold_in(own, 4), (amount // 2,), 0, 1 << 20) % (room + 1)
    tallies = tallies.at[donor].add(-passed).at[taker].add(passed)
    labels = jnp.searchsorted(jnp.cumsum(tallies), jnp.arange(rows * top), side="right").astype(jnp.int32)
    listing = labels.reshape(top, rows).T
    listing = listing[jax.random.permutation(jax.random.fold_in(own, 1), rows)]
    offset_by = jax.random.randint(jax.random.fold_in(own, 2), (rows, 1), 0, top)
    return jnp.take_along_axis(listing, (jnp.arange(top)[None, :] + offset_by) % top, axis=1)


def shares(count, total, limit, skew, full):
    portions = [(1 << 20) // math.isqrt(grade ** skew) + 1 for grade in range(1, count + 1)]
    largest = limit if full else min(limit, max(-(-total // count), total * portions[0] // sum(portions)))
    least = 1 if total - largest >= count - 1 else 0
    holding, spare = [largest] + [least] * (count - 1), total - largest - least * (count - 1)
    while spare > 0:
        free = [i for i in range(1, count) if holding[i] < largest] or [i for i in range(1, count) if holding[i] < limit]
        mass, remaining = sum([portions[i] for i in free]), spare
        for i in free:
            more = min(limit - holding[i], max(1, remaining * portions[i] // mass), spare)
            holding[i] = holding[i] + more
            spare = spare - more
    return np.array(holding)


def noise(stream_key, dims, scale, most, shards=(), held_as=jnp.bfloat16):
    entries = scale * jax.random.normal(stream_key, dims, jnp.float32)
    if shards:
        entries = entries * steps_of(stream_key, dims, shards, -0.22, 0.18)
    return jnp.clip(entries, -most, most).astype(held_as)


def setup_inputs(seed: int = 0) -> dict:
    arg_keys = jax.random.split(jax.random.key(seed), 7)
    tokens = noise(arg_keys[0], (TOKENS, D), 1.0, 6.0, ((0, 32),))
    expert_ids_keys = jax.random.split(jax.random.fold_in(arg_keys[1], 1), TOKENS // TOK_DEV)
    expert_ids_turns = jax.random.permutation(jax.random.fold_in(arg_keys[1], 3), TOKENS // TOK_DEV)
    expert_ids = jax.vmap(lambda own, number: routed_block(jax.random.fold_in(arg_keys[1], 2), own, number, TOK_DEV, EXPERTS, TOP, CAP, 2))(expert_ids_keys, expert_ids_turns).reshape((TOKENS, TOP))
    route_weights = jnp.clip(jnp.exp(math.log(0.4) - 2.5902672 * jax.random.uniform(arg_keys[2], (TOKENS, TOP), jnp.float32) ** steps_of(arg_keys[2], (TOKENS, TOP), ((0, 32),), -0.2, 0.2)), 0.03, 0.4)
    w_gate = noise(arg_keys[3], (EXPERTS, D, FFE), D ** -0.5, 0.125, ((0, 32),))
    w_up = noise(arg_keys[4], (EXPERTS, D, FFE), D ** -0.5, 0.125, ((0, 32),))
    w_down = noise(arg_keys[5], (EXPERTS, FFE, D), FFE ** -0.5, 0.21875, ((0, 32),))
    return {"tokens": tokens, "expert_ids": expert_ids, "route_weights": route_weights, "w_gate": w_gate, "w_up": w_up, "w_down": w_down}


def expert_ffn(rows, gate_proj, up_proj, down_proj):
    gate = jnp.dot(rows, gate_proj, preferred_element_type=jnp.float32)
    upper = jnp.dot(rows, up_proj, preferred_element_type=jnp.float32)
    hidden = (jax.nn.silu(gate) * upper).astype(jnp.bfloat16)
    return jnp.dot(hidden, down_proj, preferred_element_type=jnp.float32).astype(jnp.bfloat16)


def reference(tokens, expert_ids, route_weights, w_gate, w_up, w_down):
    blocks = TOKENS // TOK_DEV
    block_pairs = TOK_DEV * TOP
    flat_ids = expert_ids.reshape(blocks, block_pairs).astype(jnp.int32)
    onehot = (flat_ids[:, :, None] == jnp.arange(EXPERTS, dtype=jnp.int32)[None, None, :]).astype(jnp.int32)
    earlier = jnp.cumsum(onehot, axis=1) - onehot
    slot_index = jnp.sum(earlier * onehot, axis=2).astype(jnp.int32)
    owner = jnp.arange(blocks, dtype=jnp.int32)[:, None]
    keys = ((flat_ids * blocks + owner) * CAP + slot_index).reshape(-1).astype(jnp.int32)
    token_of = (jnp.arange(TOKENS * TOP, dtype=jnp.int32) // TOP).astype(jnp.int32)
    per_expert = blocks * CAP
    table_token = jnp.full((EXPERTS * per_expert,), -1, jnp.int32).at[keys].set(token_of)
    table_weight = jnp.zeros((EXPERTS * per_expert,), jnp.float32).at[keys].set(route_weights.reshape(-1))

    def one_expert(total, inputs):
        gate_proj, up_proj, down_proj, expert = inputs
        start = (expert * per_expert).astype(jnp.int32)
        index = lax.dynamic_slice_in_dim(table_token, start, per_expert)
        weight = lax.dynamic_slice_in_dim(table_weight, start, per_expert)
        safe = jnp.maximum(index, 0).astype(jnp.int32)
        rows = jnp.where((index >= 0)[:, None], tokens[safe], jnp.zeros((), tokens.dtype))
        output = expert_ffn(rows, gate_proj, up_proj, down_proj)
        total = total.at[safe].add(weight[:, None] * output.astype(jnp.float32))
        return total, None

    start_total = jnp.zeros((TOKENS, D), jnp.float32)
    total, _ = lax.scan(one_expert, start_total, (w_gate, w_up, w_down, jnp.arange(EXPERTS, dtype=jnp.int32)))
    return total.astype(jnp.bfloat16)
```

```python
import functools

import jax
import jax.numpy as jnp
from jax import lax
from jax.experimental import pallas as pl
from jax.experimental.pallas import tpu as pltpu
from jax.sharding import PartitionSpec as P

AXES = ("side", "lane")
MESH = pl.DeviceIdType.MESH
BF16 = jnp.bfloat16
F32 = jnp.float32


def flip(value, mask):
    bit = 1
    out = value
    while bit <= mask:
        if mask & bit:
            out = out + bit - 2 * bit * ((value // bit) % 2)
        bit *= 2
    return out


def fused_kernel(
    levels, spare, tokens, ids, gains, wg, wu, wd, out, ids_v, gains_v, mine, shares, slots, wgs, wus, wds, every,
    part, xs, ys, backs, first, second, row_in, plane_in, gs, gr, zs, zr, bs, br, ps, pr, cs, cr, ds, dr, ss, sr, ws,
    wr, local
):
    side, level = lax.axis_index("side"), lax.axis_index("lane")
    col, core = side // 2, side % 2
    mid = ((level + 1) // 2) % 2
    rows = out.shape[0]
    width = out.shape[1]
    chips = shares.shape[0]
    columns = chips // levels
    cap = xs.shape[1] // columns
    main = rows - spare
    cut = (main // 2 + 15) // 16 * 16
    bcut = spare // 2
    whole = (pl.ds(0, rows // 2), pl.ds(rows // 2, rows // 2))
    part_rows = (pl.ds(0, cut), pl.ds(cut, main - cut))
    tail_rows = (pl.ds(main, bcut), pl.ds(main + bcut, spare - bcut))
    tail = pl.ds(main, spare)
    dev_x, dev_y = (flip(col, 1) * 2 + core, level), (flip(col, 2) * 2 + core, level)
    twin = (col * 2 + 1 - core, level)
    mate = (side, flip(level, 1))
    inner = (side, mid * flip(level, 3) + (1 - mid) * flip(level, 1))
    lev = [
        level,
        flip(level, 1),
        mid * flip(level, 3) + (1 - mid) * flip(level, 2),
        mid * flip(level, 2) + (1 - mid) * flip(level, 3),
    ]
    me = col * levels + level
    others = [(flip(col, m // levels), flip(level, m % levels)) for m in range(1, chips)]

    fetch = [pltpu.make_async_copy(ids, ids_v, local.at[0]), pltpu.make_async_copy(gains, gains_v, local.at[1])]
    for copy in fetch:
        copy.start()
    barrier = pltpu.get_barrier_semaphore()
    friends = [(q * 2 + core, z) for q, z in others] + [twin]
    for device in friends:
        pl.semaphore_signal(barrier, inc=1, device_id=device, device_id_type=MESH)
    keep = [
        pltpu.make_async_copy(tokens, every.at[0, 0], local.at[2]),
        pltpu.make_async_copy(wg.at[0], wgs.at[0], local.at[3]),
        pltpu.make_async_copy(wu.at[0], wus.at[0], local.at[4]),
        pltpu.make_async_copy(wd.at[0], wds.at[0], local.at[5]),
    ]
    for copy in keep:
        copy.start()
    for copy in fetch:
        copy.wait()
    number = lax.broadcasted_iota(jnp.int32, (rows, 128), 1)
    table = jnp.zeros((rows, 128), F32)
    for k in range(ids_v.shape[1]):
        table = table + jnp.where(ids_v[:, k : k + 1] == number, gains_v[:, k : k + 1], 0.0)
    table = table.T
    for q in range(columns):
        for z in range(levels):
            for c in range(2):
                e = (q * 2 + c) * levels + z
                mine[q * levels + z, c : c + 1, :] = table[e : e + 1, :]
            mine[q * levels + z, 2:8, :] = jnp.zeros((6, rows), F32)
    shares[me] = mine[me]
    pl.semaphore_wait(barrier, len(friends))

    def link(src, dst, s, r, device):
        return pltpu.make_async_remote_copy(
            src_ref=src, dst_ref=dst, send_sem=s, recv_sem=r, device_id=device, device_id_type=MESH
        )

    def on_mid(do):
        pl.when(mid == 1)(do)

    def on_end(do):
        pl.when(mid == 0)(do)

    def spread_copies(k):
        p, q = whole if k == 0 else part_rows
        block = tokens if k == 0 else every.at[k, 0]
        return [
            link(block.at[p], every.at[k, 1, p], gs.at[k, 0], gr.at[k, 0], dev_x),
            link(block.at[q], every.at[k, 2, q], gs.at[k, 1], gr.at[k, 1], dev_y),
            link(block.at[q], every.at[k, 1, q], gs.at[k, 2], gr.at[k, 2], dev_x),
            link(block.at[p], every.at[k, 2, p], gs.at[k, 3], gr.at[k, 3], dev_y),
            link(every.at[k, 1, p], every.at[k, 3, p], gs.at[k, 4], gr.at[k, 4], dev_y),
            link(every.at[k, 2, q], every.at[k, 3, q], gs.at[k, 5], gr.at[k, 5], dev_x),
        ]

    spread = [spread_copies(k) for k in range(levels)]

    def spread_send(k):
        for i in range(4):
            spread[k][i].start()

    def spread_relay(k):
        spread[k][0].wait_recv()
        spread[k][4].start()
        spread[k][1].wait_recv()
        spread[k][5].start()

    def spread_done(k):
        for i in range(2, 6):
            spread[k][i].wait_recv()

    def line_copies(view, own, s, r):
        return [
            link(own, view(1), s.at[0], r.at[1], mate),
            link(own, view(2), s.at[1], r.at[2], inner),
            link(view(1), view(3), s.at[2], r.at[3], inner),
            link(view(2), view(2), s.at[3], r.at[2], mate),
            link(view(3), view(3), s.at[4], r.at[3], mate),
        ]

    lines = line_copies(lambda k: every.at[k, 0], tokens, zs, zr)

    def tails(k):
        return every.at[k, pl.ds(1, columns - 1), tail]

    bands = line_copies(tails, tails(0), bs, br)

    def line_wait(copies, k):
        copies[(0, 0, 1, 2)[k]].wait_recv()

    def line_send(copies):
        copies[0].start()
        on_mid(copies[1].start)

    def line_relay(copies, k):
        line_wait(copies, k)
        copies[k + 1].start()

    small = [
        link(mine.at[q * levels + z], shares.at[me], ss.at[i], sr.at[i], (q * 2 + core, z))
        for i, (q, z) in enumerate(others)
    ]
    swap = [
        link(wg.at[0], wgs.at[1], ws.at[0], wr.at[0], twin),
        link(wu.at[0], wus.at[1], ws.at[1], wr.at[1], twin),
        link(wd.at[0], wds.at[1], ws.at[2], wr.at[2], twin),
    ]

    def make_slots():
        chosen = (shares[...] > 0.0).astype(F32).astype(BF16).reshape(chips * 8, rows)
        before = lax.broadcasted_iota(jnp.int32, (rows, rows), 0) < lax.broadcasted_iota(
            jnp.int32, (rows, rows), 1
        )
        before = before.astype(F32).astype(BF16)
        slots[...] = jnp.dot(chosen, before, preferred_element_type=F32).reshape(chips, 8, rows)

    def compute(k, middle):
        place = lax.broadcasted_iota(jnp.int32, (cap, rows), 0).astype(F32)

        def pick(r, carry):
            b = (((col // 2 + r // 2) % 2) * 2 + (col + r) % 2) * levels + lev[k]
            gain, slot = shares[b], slots[b]
            wanted = []
            for e in range(2):
                g = jnp.where(core == 0, gain[e : e + 1], gain[1 - e : 2 - e])
                s = jnp.where(core == 0, slot[e : e + 1], slot[1 - e : 2 - e])
                wanted.append(jnp.where(s == place, g, 0.0))
            weights = jnp.concatenate(wanted, axis=0)
            chosen = jnp.where(weights > 0.0, 1.0, 0.0).astype(BF16)
            backs[r] = weights.T.astype(BF16)
            picked = jnp.dot(chosen, every[k, r], preferred_element_type=F32).astype(BF16)
            at = pl.ds(pl.multiple_of(r * cap, cap), cap)
            for e in range(2):
                xs[e, at] = picked[e * cap : (e + 1) * cap]
            return carry

        lax.fori_loop(0, columns, pick, 0)

        def expert(e, carry):
            @pl.when(e == 1)
            def _():
                middle()

            x = xs[e]
            gate = jnp.dot(x, wgs[e], preferred_element_type=F32)
            upper = jnp.dot(x, wus[e], preferred_element_type=F32)
            hidden = (gate / (1.0 + jnp.exp(-gate)) * upper).astype(BF16)
            ys[e] = jnp.dot(hidden, wds[e], preferred_element_type=F32).astype(BF16)
            return carry

        lax.fori_loop(0, 2, expert, 0)

        def mix(r, carry):
            at = pl.ds(pl.multiple_of(r * cap, cap), cap)
            y = jnp.concatenate([ys[e, at] for e in range(2)], axis=0)
            part[k, r] = jnp.dot(backs[r], y, preferred_element_type=F32).astype(BF16)
            return carry

        lax.fori_loop(0, columns, mix, 0)

    def fold_copies(g):
        k = g % levels
        p, q = part_rows if g < levels else tail_rows
        a, b = pl.ds(0, p.size), pl.ds(0, q.size)
        return [
            link(part.at[k, 3, p], first.at[g, 0, a], ps.at[g, 0], pr.at[g, 0], dev_x),
            link(part.at[k, 3, q], first.at[g, 1, b], ps.at[g, 1], pr.at[g, 1], dev_y),
            link(part.at[k, 1, p], first.at[g, 2, a], ps.at[g, 2], pr.at[g, 2], dev_x),
            link(part.at[k, 2, q], first.at[g, 3, b], ps.at[g, 3], pr.at[g, 3], dev_y),
            link(part.at[k, 2, p], second.at[g, 0, a], ps.at[g, 4], pr.at[g, 4], dev_y),
            link(part.at[k, 1, q], second.at[g, 1, b], ps.at[g, 5], pr.at[g, 5], dev_x),
        ]

    folds = [fold_copies(g) for g in range(levels + 1)]

    def fold_one(g):
        for i in range(4):
            folds[g][i].start()

    def fold_two(g):
        k = g % levels
        p, q = part_rows if g < levels else tail_rows
        for i, (r, piece) in enumerate(((2, p), (1, q))):
            folds[g][i].wait_recv()
            part[k, r, piece] = (
                part[k, r, piece].astype(F32) + first[g, i, pl.ds(0, piece.size)].astype(F32)
            ).astype(BF16)
            folds[g][4 + i].start()

    def fold_sum(g, i):
        k = g % levels
        piece = (part_rows if g < levels else tail_rows)[i]
        at = pl.ds(0, piece.size)
        return (
            part[k, 0, piece].astype(F32) + first[g, 2 + i, at].astype(F32) + second[g, i, at].astype(F32)
        )

    def fold_three(g, store):
        for i in range(2):
            folds[g][2 + i].wait_recv()
            folds[g][4 + i].wait_recv()
            store(i, fold_sum(g, i))

    def keep_sum(k):
        def store(i, value):
            part[k, 0, part_rows[i]] = value.astype(BF16)

        return store

    def chain(view, land, s, r):
        send_end = {
            3: link(view(3), land.at[3], s.at[3], r.at[3], mate),
            2: link(view(2), land.at[2], s.at[2], r.at[2], mate),
            1: link(view(1), land.at[0], s.at[1], r.at[0], mate),
        }
        send_mid = {
            3: link(view(3), land.at[4], s.at[3], r.at[4], inner),
            2: link(view(2), land.at[1], s.at[2], r.at[1], inner),
            1: send_end[1],
        }
        return send_end, send_mid, {3: 3, 2: 2, 1: 4}

    def main_view(k):
        return part.at[k, 0, pl.ds(0, main)]

    def tail_view(k):
        return part.at[k, pl.ds(0, columns), tail]

    rows_chain = chain(main_view, row_in, cs, cr)
    tail_chain = chain(tail_view, plane_in, ds, dr)

    def landed(land, r, slot):
        link(land.at[slot], land.at[slot], r.at[slot], r.at[slot], mate).wait_recv()

    def chain_end(c, k):
        on_end(c[0][k].start)

    def chain_mid(c, view, land, r, k):
        def do():
            slot = c[2][k]
            landed(land, r, slot)
            here = view(k)
            here[...] = (here[...].astype(F32) + land[slot].astype(F32)).astype(BF16)
            c[1][k].start()

        on_mid(do)

    def main_end(k):
        chain_end(rows_chain, k)

    def main_mid(k):
        chain_mid(rows_chain, main_view, row_in, cr, k)

    def tail_end(k):
        chain_end(tail_chain, k)

    def tail_mid(k):
        chain_mid(tail_chain, tail_view, plane_in, dr, k)

    spread[0][0].start()
    spread[0][1].start()
    line_send(lines)
    for copy in small:
        copy.start()
    spread[0][2].start()
    spread[0][3].start()
    for copy in swap:
        copy.start()
    spread_relay(0)
    line_wait(lines, 1)
    on_mid(lines[2].start)
    spread_send(1)
    on_mid(lambda: line_relay(lines, 2))
    for copy in small:
        copy.wait_recv()
    make_slots()
    spread_done(0)
    line_send(bands)
    for copy in keep:
        copy.wait()

    def hook_0():
        spread_relay(1)
        on_mid(lambda: line_relay(lines, 3))
        for copy in swap:
            copy.wait_recv()

    compute(0, hook_0)
    on_end(lambda: line_wait(lines, 2))
    spread_send(2)
    line_wait(bands, 1)
    on_mid(bands[2].start)
    spread_done(1)

    def hook_1():
        spread_relay(2)
        on_mid(lambda: line_relay(bands, 2))

    compute(1, hook_1)
    tail_end(1)
    on_end(lambda: line_wait(lines, 3))
    spread_send(3)
    on_mid(lambda: line_relay(bands, 3))
    spread_done(2)
    on_end(lambda: line_wait(bands, 2))

    def hook_2():
        spread_relay(3)
        fold_one(1)

    compute(2, hook_2)
    tail_end(2)
    spread_done(3)
    on_end(lambda: line_wait(bands, 3))

    def hook_3():
        fold_two(1)

    compute(3, hook_3)
    fold_one(3)
    tail_end(3)
    fold_two(3)
    tail_mid(2)
    fold_one(2)
    fold_three(3, keep_sum(3))
    main_end(3)
    tail_mid(3)
    fold_three(1, keep_sum(1))
    main_end(1)
    fold_two(2)
    fold_one(0)
    main_mid(3)
    fold_three(2, keep_sum(2))
    main_end(2)
    tail_mid(1)
    fold_two(0)
    main_mid(2)
    landed(plane_in, dr, 0)
    on_mid(lambda: landed(plane_in, dr, 1))

    def own(land, extra):
        return land[0].astype(F32) + jnp.where(mid == 1, land[1].astype(F32), 0.0)

    for r in range(columns):
        part[0, r, tail] = (part[0, r, tail].astype(F32) + own(plane_in.at[:, r], r)).astype(BF16)
    fold_one(levels)
    main_mid(1)
    fold_two(levels)
    landed(row_in, cr, 0)
    on_mid(lambda: landed(row_in, cr, 1))

    def main_out(i, value):
        piece = part_rows[i]
        total = value + row_in[0, piece].astype(F32) + jnp.where(mid == 1, row_in[1, piece].astype(F32), 0.0)
        out[piece] = total.astype(BF16)

    def tail_out(i, value):
        out[tail_rows[i]] = value.astype(BF16)

    fold_three(0, main_out)
    fold_three(levels, tail_out)

    for group in spread + folds + [small, swap]:
        for copy in group:
            copy.wait_send()
    for copies in (lines, bands):
        copies[0].wait_send()
    for c in (rows_chain, tail_chain):
        c[0][1].wait_send()

    @pl.when(mid == 1)
    def _():
        for copies in (lines, bands):
            for copy in copies[1:]:
                copy.wait_send()
        for c in (rows_chain, tail_chain):
            c[1][2].wait_send()
            c[1][3].wait_send()

    @pl.when(mid == 0)
    def _():
        for c in (rows_chain, tail_chain):
            c[0][2].wait_send()
            c[0][3].wait_send()


def on_layers(levels, tokens, expert_ids, route_weights, w_gate, w_up, w_down):
    tok_rows, width = tokens.shape
    top_count = expert_ids.shape[1]
    device_count = lax.axis_size("side") * levels
    capacity = 2 * tok_rows * top_count // device_count
    chips = device_count // 2
    columns = chips // levels
    spare = tok_rows // 4
    main = tok_rows - spare
    cut = (main // 2 + 15) // 16 * 16
    anywhere = pl.BlockSpec(memory_space=pl.ANY)
    vmem = pltpu.VMEM
    dma = pltpu.SemaphoreType.DMA
    return pl.pallas_call(
        functools.partial(fused_kernel, levels, spare),
        out_shape=jax.ShapeDtypeStruct((tok_rows, width), BF16),
        in_specs=[anywhere] * 6,
        out_specs=pl.BlockSpec(memory_space=vmem),
        scratch_shapes=[
            vmem(expert_ids.shape, jnp.int32),
            vmem(route_weights.shape, F32),
            vmem((chips, 8, tok_rows), F32),
            vmem((chips, 8, tok_rows), F32),
            vmem((chips, 8, tok_rows), F32),
            vmem((2,) + w_gate.shape[1:], BF16),
            vmem((2,) + w_up.shape[1:], BF16),
            vmem((2,) + w_down.shape[1:], BF16),
            vmem((levels, columns, tok_rows, width), BF16),
            vmem((levels, columns, tok_rows, width), BF16),
            vmem((2, columns * capacity, width), BF16),
            vmem((2, columns * capacity, width), BF16),
            vmem((columns, tok_rows, 2 * capacity), BF16),
            vmem((levels + 1, 4, cut, width), BF16),
            vmem((levels + 1, 2, cut, width), BF16),
            vmem((5, main, width), BF16),
            vmem((5, columns, spare, width), BF16),
            dma((levels, 6)),
            dma((levels, 6)),
            dma((5,)),
            dma((4,)),
            dma((5,)),
            dma((4,)),
            dma((levels + 1, 6)),
            dma((levels + 1, 6)),
            dma((4,)),
            dma((5,)),
            dma((4,)),
            dma((5,)),
            dma((chips - 1,)),
            dma((chips - 1,)),
            dma((3,)),
            dma((3,)),
            dma((6,)),
        ],
        compiler_params=pltpu.CompilerParams(
            collective_id=0, has_side_effects=True, vmem_limit_bytes=62 * 2**20
        ),
        name="layer",
    )(tokens, expert_ids, route_weights, w_gate, w_up, w_down)


def expert_ffn(rows, gate_proj, up_proj, down_proj):
    gate = jnp.dot(rows, gate_proj, preferred_element_type=jnp.float32)
    upper = jnp.dot(rows, up_proj, preferred_element_type=jnp.float32)
    hidden = (jax.nn.silu(gate) * upper).astype(jnp.bfloat16)
    return jnp.dot(hidden, down_proj, preferred_element_type=jnp.float32).astype(jnp.bfloat16)


def on_device(tokens, expert_ids, route_weights, w_gate, w_up, w_down):
    tok_rows = tokens.shape[0]
    width = tokens.shape[1]
    top_count = expert_ids.shape[1]
    side_count = lax.axis_size("side")
    device_count = side_count * lax.axis_size("lane")
    local_count = w_gate.shape[0]
    expert_count = device_count * local_count
    capacity = 2 * tok_rows * top_count // expert_count
    flat_ids = expert_ids.reshape(-1)
    onehot = (flat_ids[:, None] == jnp.arange(expert_count, dtype=jnp.int32)[None, :]).astype(
        jnp.int32
    )
    earlier = jnp.cumsum(onehot, axis=0) - onehot
    slot_index = jnp.sum(earlier * onehot, axis=1)
    position = (flat_ids * capacity + slot_index).reshape(tok_rows, top_count)
    buffer_rows = jnp.arange(expert_count * capacity, dtype=jnp.int32)
    dispatch_table = jnp.any(buffer_rows[:, None, None] == position[None, :, :], axis=2).astype(
        jnp.bfloat16
    )
    outgoing = jnp.dot(dispatch_table, tokens, preferred_element_type=jnp.float32).astype(
        jnp.bfloat16
    )
    outgoing = outgoing.reshape(expert_count, capacity, width)
    received = lax.all_to_all(outgoing, ("side", "lane"), split_axis=0, concat_axis=0, tiled=True)
    count = received.shape[1]
    grouped = received.reshape(device_count, local_count, count, width)
    rows = grouped[:, 0].reshape(device_count * count, width)
    output = expert_ffn(rows, w_gate[0], w_up[0], w_down[0])
    results = [output.reshape(device_count, count, width)]
    returned = lax.all_to_all(
        jnp.stack(results, axis=1).reshape(device_count * local_count, count, width),
        ("side", "lane"),
        split_axis=0,
        concat_axis=0,
        tiled=True,
    )
    flat_back = returned.reshape(expert_count * capacity, width)
    picked = flat_back[position]
    mixed = jnp.einsum("tk,tkd->td", route_weights, picked, preferred_element_type=jnp.float32)
    return mixed.astype(jnp.bfloat16)


def layered(mesh, tokens):
    side, levels = mesh.shape["side"], mesh.shape["lane"]
    layer_bytes = tokens.shape[0] // 2 * tokens.shape[1] * tokens.dtype.itemsize
    fits = 3 * layer_bytes < 32 * 2**20 and side * levels <= tokens.shape[0] // (side * levels) == 2**7
    return side == 2**3 and levels == 4 and fits


def solution(mesh):
    placed = (
        P(AXES, None),
        P(AXES, None),
        P(AXES, None),
        P(AXES, None, None),
        P(AXES, None, None),
        P(AXES, None, None),
    )

    def run(tokens, *rest):
        body = on_device
        if layered(mesh, tokens):
            body = functools.partial(on_layers, mesh.shape["lane"])
        return jax.shard_map(
            body, mesh=mesh, in_specs=placed, out_specs=P(AXES, None), check_vma=False
        )(tokens, *rest)

    return run
```

```python
import functools

import jax
import jax.numpy as jnp
from jax import lax
from jax.experimental import pallas as pl
from jax.experimental.pallas import tpu as pltpu
from jax.sharding import PartitionSpec as P

AXES = ("side", "lane")
MESH = pl.DeviceIdType.MESH
BF16 = jnp.bfloat16
F32 = jnp.float32


ORDER = [
    ("all", "Start"), ("end", "Sr", 0), ("end", "Lw", 1), ("end", "Ss", 1), ("end", "T"),
    ("end", "Sd", 0), ("end", "Bs"), ("mid", "Sr", 0), ("mid", "Lr", 2, 0), ("mid", "Lr", 1, 0),
    ("mid", "Lr", 2, 1), ("mid", "Ss", 2), ("mid", "Lr", 1, 1), ("mid", "Sd", 0), ("mid", "T"),
    ("mid", "Ss", 1), ("mid", "Bs"), ("mid", "Bi"), ("mid", "Br", 1, 0), ("mid", "Lr", 3, 1),
    ("mid", "Lr", 3, 0), ("mid", "Sr", 1),
    ("all", "C", 0, [
        ("end", "Sr", 1), ("end", "Lw", 2), ("mid", "Sr", 2), ("mid", "Ss", 3), ("mid", "Br", 2, 1),
        ("all", "Swap"),
    ]),
    ("end", "Ss", 2), ("end", "Bw", 1), ("end", "Sd", 1), ("end", "Sr", 2), ("mid", "Br", 2, 0),
    ("mid", "Sd", 1), ("mid", "Br", 1, 1),
    ("all", "C", 1, [
        ("mid", "Br", 3, 0), ("mid", "Br", 3, 1),
    ]),
    ("end", "Lw", 3), ("end", "Ss", 3), ("end", "De", 1, 0), ("end", "De", 1, 1), ("end", "Bw", 2),
    ("end", "Sr", 3), ("end", "Sd", 2), ("end", "F1", 1), ("mid", "Sr", 3), ("mid", "F1", 1),
    ("mid", "Sd", 2),
    ("all", "C", 2, [
        ("mid", "F2", 1), ("mid", "Sd", 3),
    ]),
    ("end", "Sd", 3), ("end", "De", 2, 0), ("end", "De", 2, 1), ("end", "Bw", 3), ("mid", "F1", 2),
    ("all", "C", 3, [
        ("end", "F2", 1), ("mid", "Dm", 2, 0),
    ]),
    ("end", "De", 3, 0), ("end", "F1", 3), ("end", "De", 3, 1), ("end", "F2", 3), ("end", "F1", 2),
    ("end", "F3", 3, 0), ("end", "Ce", 3, 0), ("end", "F3", 1, 0), ("end", "F3", 1, 1),
    ("end", "F3", 3, 1), ("end", "Ce", 3, 1), ("end", "F2", 2), ("end", "F1", 0), ("end", "Ce", 1, 0),
    ("end", "Dw", 0), ("end", "F3", 2, 0), ("end", "Ce", 2, 0), ("end", "F3", 2, 1),
    ("end", "Ce", 2, 1), ("end", "Dw", 1), ("end", "F1", 4), ("end", "Ce", 1, 1), ("end", "F2", 0),
    ("end", "Cw", 1), ("end", "F2", 4), ("end", "F3", 0, 0), ("end", "Cw", 0), ("end", "F3", 0, 1),
    ("end", "F3", 4, 0), ("end", "F3", 4, 1), ("mid", "F1", 3), ("mid", "Dm", 2, 1),
    ("mid", "Dm", 3, 0), ("mid", "F3", 1, 0), ("mid", "Dw", 0), ("mid", "F2", 3), ("mid", "Dm", 3, 1),
    ("mid", "Dw", 1), ("mid", "F1", 4), ("mid", "Dm", 1, 0), ("mid", "F3", 1, 1), ("mid", "F2", 2),
    ("mid", "F3", 3, 1), ("mid", "F3", 3, 0), ("mid", "Dm", 1, 1), ("mid", "Cm", 3, 1),
    ("mid", "F1", 0), ("mid", "Cm", 3, 0), ("mid", "F2", 4), ("mid", "F3", 2, 0), ("mid", "F2", 0),
    ("mid", "Cm", 1, 1), ("mid", "Cm", 2, 0), ("mid", "Cm", 1, 0), ("mid", "F3", 2, 1),
    ("mid", "Cm", 2, 1), ("mid", "F3", 4, 0), ("mid", "F3", 4, 1), ("mid", "F3", 0, 1),
    ("mid", "Cw", 0), ("mid", "F3", 0, 0), ("mid", "Cw", 1),
]


def flip(value, mask):
    bit = 1
    out = value
    while bit <= mask:
        if mask & bit:
            out = out + bit - 2 * bit * ((value // bit) % 2)
        bit *= 2
    return out


def fused_kernel(
    levels, spare, tokens, ids, gains, wg, wu, wd, out, ids_v, gains_v, mine, shares, slots, wgs, wus, wds, every,
    part, xs, ys, backs, first, second, row_in, plane_in, gs, gr, zs, zr, bs, br, ps, pr, cs, cr, ds, dr, ss, sr, ws,
    wr, local
):
    side, level = lax.axis_index("side"), lax.axis_index("lane")
    col, core = side // 2, side % 2
    mid = ((level + 1) // 2) % 2
    rows = out.shape[0]
    width = out.shape[1]
    chips = shares.shape[0]
    columns = chips // levels
    cap = xs.shape[1] // columns
    main = rows - spare
    cut = (main // 2 + 15) // 16 * 16
    bcut = spare // 2
    whole = (pl.ds(0, rows // 2), pl.ds(rows // 2, rows // 2))
    part_rows = (pl.ds(0, cut), pl.ds(cut, main - cut))
    tail_rows = (pl.ds(main, bcut), pl.ds(main + bcut, spare - bcut))
    dev_x, dev_y = (flip(col, 1) * 2 + core, level), (flip(col, 2) * 2 + core, level)
    twin = (col * 2 + 1 - core, level)
    mate = (side, flip(level, 1))
    inner = (side, mid * flip(level, 3) + (1 - mid) * flip(level, 1))
    lev = [
        level,
        flip(level, 1),
        mid * flip(level, 3) + (1 - mid) * flip(level, 2),
        mid * flip(level, 2) + (1 - mid) * flip(level, 3),
    ]
    me = col * levels + level
    others = [(flip(col, m // levels), flip(level, m % levels)) for m in range(1, chips)]

    fetch = [pltpu.make_async_copy(ids, ids_v, local.at[0]), pltpu.make_async_copy(gains, gains_v, local.at[1])]
    for copy in fetch:
        copy.start()
    barrier = pltpu.get_barrier_semaphore()
    friends = [(q * 2 + core, z) for q, z in others] + [twin]
    for device in friends:
        pl.semaphore_signal(barrier, inc=1, device_id=device, device_id_type=MESH)
    keep = [
        pltpu.make_async_copy(tokens, every.at[0, 0], local.at[2]),
        pltpu.make_async_copy(wg.at[0], wgs.at[0], local.at[3]),
        pltpu.make_async_copy(wu.at[0], wus.at[0], local.at[4]),
        pltpu.make_async_copy(wd.at[0], wds.at[0], local.at[5]),
    ]
    for copy in keep:
        copy.start()
    for copy in fetch:
        copy.wait()
    number = lax.broadcasted_iota(jnp.int32, (2 * chips, rows), 0)
    table = jnp.zeros((2 * chips, rows), F32)
    for k in range(ids_v.shape[0]):
        table = table + jnp.where(ids_v[k : k + 1] == number, gains_v[k : k + 1], 0.0)
    for q in range(columns):
        for z in range(levels):
            for c in range(2):
                e = (q * 2 + c) * levels + z
                mine[q * levels + z, c : c + 1, :] = table[e : e + 1, :]
            mine[q * levels + z, 2:8, :] = jnp.zeros((6, rows), F32)
    shares[me] = mine[me]
    pl.semaphore_wait(barrier, len(friends))

    def link(src, dst, s, r, device):
        return pltpu.make_async_remote_copy(
            src_ref=src, dst_ref=dst, send_sem=s, recv_sem=r, device_id=device, device_id_type=MESH
        )

    def on_mid(do):
        pl.when(mid == 1)(do)

    def on_end(do):
        pl.when(mid == 0)(do)

    def spread_copies(k):
        p, q = whole if k == 0 else part_rows
        block = tokens if k == 0 else every.at[k, 0]
        return [
            link(block.at[p], every.at[k, 1, p], gs.at[k, 0], gr.at[k, 0], dev_x),
            link(block.at[q], every.at[k, 2, q], gs.at[k, 1], gr.at[k, 1], dev_y),
            link(block.at[q], every.at[k, 1, q], gs.at[k, 2], gr.at[k, 2], dev_x),
            link(block.at[p], every.at[k, 2, p], gs.at[k, 3], gr.at[k, 3], dev_y),
            link(every.at[k, 1, p], every.at[k, 3, p], gs.at[k, 4], gr.at[k, 4], dev_y),
            link(every.at[k, 2, q], every.at[k, 3, q], gs.at[k, 5], gr.at[k, 5], dev_x),
        ]

    spread = [spread_copies(k) for k in range(levels)]

    def spread_send(k):
        for i in range(4):
            spread[k][i].start()

    def spread_relay(k):
        spread[k][0].wait_recv()
        spread[k][4].start()
        spread[k][1].wait_recv()
        spread[k][5].start()

    def spread_done(k):
        for i in range(2, 6):
            spread[k][i].wait_recv()

    def line_copies(view, own, s, r):
        out = []
        for i in range(2):
            out.append(
                [
                    link(own(i), view(1, i), s.at[0, i], r.at[1, i], mate),
                    link(own(i), view(2, i), s.at[1, i], r.at[2, i], inner),
                    link(view(1, i), view(3, i), s.at[2, i], r.at[3, i], inner),
                    link(view(2, i), view(2, i), s.at[3, i], r.at[2, i], mate),
                    link(view(3, i), view(3, i), s.at[4, i], r.at[3, i], mate),
                ]
            )
        return out

    block_rows = (pl.ds(0, cut), pl.ds(cut, rows - cut))
    lines = line_copies(
        lambda k, i: every.at[k, 0, block_rows[i]], lambda i: tokens.at[block_rows[i]], zs, zr
    )

    def tails(k, i):
        return every.at[k, pl.ds(1, columns - 1), tail_rows[i]]

    bands = line_copies(tails, lambda i: tails(0, i), bs, br)

    def line_send(copies):
        for i in range(2):
            copies[i][0].start()

    def line_send_inner(copies):
        for i in range(2):
            copies[i][1].start()

    def line_wait(copies, k):
        for i in range(2):
            copies[i][k - 1].wait_recv()

    def line_relay(copies, k, i):
        copies[i][k - 1].wait_recv()
        copies[i][k + 1].start()

    small = [
        link(mine.at[q * levels + z], shares.at[me], ss.at[i], sr.at[i], (q * 2 + core, z))
        for i, (q, z) in enumerate(others)
    ]
    swap = [
        link(wg.at[0], wgs.at[1], ws.at[0], wr.at[0], twin),
        link(wu.at[0], wus.at[1], ws.at[1], wr.at[1], twin),
        link(wd.at[0], wds.at[1], ws.at[2], wr.at[2], twin),
    ]

    def make_slots():
        chosen = (shares[...] > 0.0).astype(F32).astype(BF16).reshape(chips * 8, rows)
        before = lax.broadcasted_iota(jnp.int32, (rows, rows), 0) < lax.broadcasted_iota(
            jnp.int32, (rows, rows), 1
        )
        before = before.astype(F32).astype(BF16)
        slots[...] = jnp.dot(chosen, before, preferred_element_type=F32).reshape(chips, 8, rows)

    def compute(k, middle):
        place = lax.broadcasted_iota(jnp.int32, (cap, rows), 0).astype(F32)

        def pick(r, carry):
            b = (((col // 2 + r // 2) % 2) * 2 + (col + r) % 2) * levels + lev[k]
            gain, slot = shares[b], slots[b]
            wanted = []
            for e in range(2):
                g = jnp.where(core == 0, gain[e : e + 1], gain[1 - e : 2 - e])
                s = jnp.where(core == 0, slot[e : e + 1], slot[1 - e : 2 - e])
                wanted.append(jnp.where(s == place, g, 0.0))
            weights = jnp.concatenate(wanted, axis=0)
            chosen = jnp.where(weights > 0.0, 1.0, 0.0).astype(BF16)
            backs[r] = weights.T.astype(BF16)
            picked = jnp.dot(chosen, every[k, r], preferred_element_type=F32).astype(BF16)
            at = pl.ds(pl.multiple_of(r * cap, cap), cap)
            for e in range(2):
                xs[e, at] = picked[e * cap : (e + 1) * cap]
            return carry

        lax.fori_loop(0, columns, pick, 0)

        def expert(e, carry):
            @pl.when(e == 1)
            def _():
                middle()

            x = xs[e]
            gate = jnp.dot(x, wgs[e], preferred_element_type=F32)
            upper = jnp.dot(x, wus[e], preferred_element_type=F32)
            hidden = (gate / (1.0 + jnp.exp(-gate)) * upper).astype(BF16)
            ys[e] = jnp.dot(hidden, wds[e], preferred_element_type=F32).astype(BF16)
            return carry

        lax.fori_loop(0, 2, expert, 0)

        def mix(r, carry):
            at = pl.ds(pl.multiple_of(r * cap, cap), cap)
            y = jnp.concatenate([ys[e, at] for e in range(2)], axis=0)
            part[k, r] = jnp.dot(backs[r], y, preferred_element_type=F32).astype(BF16)
            return carry

        lax.fori_loop(0, columns, mix, 0)

    def fold_copies(g):
        k = g % levels
        p, q = part_rows if g < levels else tail_rows
        a, b = pl.ds(0, p.size), pl.ds(0, q.size)
        return [
            link(part.at[k, 3, p], first.at[g, 0, a], ps.at[g, 0], pr.at[g, 0], dev_x),
            link(part.at[k, 3, q], first.at[g, 1, b], ps.at[g, 1], pr.at[g, 1], dev_y),
            link(part.at[k, 1, p], first.at[g, 2, a], ps.at[g, 2], pr.at[g, 2], dev_x),
            link(part.at[k, 2, q], first.at[g, 3, b], ps.at[g, 3], pr.at[g, 3], dev_y),
            link(part.at[k, 2, p], second.at[g, 0, a], ps.at[g, 4], pr.at[g, 4], dev_y),
            link(part.at[k, 1, q], second.at[g, 1, b], ps.at[g, 5], pr.at[g, 5], dev_x),
        ]

    folds = [fold_copies(g) for g in range(levels + 1)]

    def fold_one(g):
        for i in range(4):
            folds[g][i].start()

    def fold_two(g):
        k = g % levels
        p, q = part_rows if g < levels else tail_rows
        for i, (r, piece) in enumerate(((2, p), (1, q))):
            folds[g][i].wait_recv()
            part[k, r, piece] = (
                part[k, r, piece].astype(F32) + first[g, i, pl.ds(0, piece.size)].astype(F32)
            ).astype(BF16)
            folds[g][4 + i].start()

    def fold_wait(g, i):
        folds[g][2 + i].wait_recv()
        folds[g][4 + i].wait_recv()

    def fold_sum(g, i):
        k = g % levels
        piece = (part_rows if g < levels else tail_rows)[i]
        at = pl.ds(0, piece.size)
        return (
            part[k, 0, piece].astype(F32) + first[g, 2 + i, at].astype(F32) + second[g, i, at].astype(F32)
        )

    def fold_three(g, i):
        fold_wait(g, i)
        if g == levels:
            out[tail_rows[i]] = fold_sum(g, i).astype(BF16)
        elif g:
            part[g, 0, part_rows[i]] = fold_sum(g, i).astype(BF16)

    def chain(view, land, s, r):
        send_end, send_mid = {}, {}
        for i in range(2):
            for k, end_slot, mid_slot in ((3, 3, 4), (2, 2, 1), (1, 0, 0)):
                send_end[k, i] = link(view(k, i), land(end_slot, i), s.at[k, i], r.at[end_slot, i], mate)
                send_mid[k, i] = link(
                    view(k, i), land(mid_slot, i), s.at[k, i], r.at[mid_slot, i], mate if k == 1 else inner
                )
        return send_end, send_mid, view, land, r

    def main_view(k, i):
        return part.at[k, 0, part_rows[i]]

    def tail_view(k, i):
        return part.at[k, pl.ds(0, columns), tail_rows[i]]

    rows_chain = chain(main_view, lambda slot, i: row_in.at[slot, part_rows[i]], cs, cr)
    tail_chain = chain(
        tail_view,
        lambda slot, i: plane_in.at[slot, pl.ds(0, columns), (pl.ds(0, bcut), pl.ds(bcut, spare - bcut))[i]],
        ds,
        dr,
    )

    def landed(c, slot, i):
        land, r = c[3], c[4]
        link(land(slot, i), land(slot, i), r.at[slot, i], r.at[slot, i], mate).wait_recv()

    def chain_mid(c, k, i):
        slot = {3: 3, 2: 2, 1: 4}[k]
        landed(c, slot, i)
        here = c[2](k, i)
        here[...] = (here[...].astype(F32) + c[3](slot, i)[...].astype(F32)).astype(BF16)
        c[1][k, i].start()

    def own_wait(c, i):
        landed(c, 0, i)

        @pl.when(mid == 1)
        def _():
            landed(c, 1, i)

    def own_rows(c, i):
        return c[3](0, i)[...].astype(F32) + jnp.where(mid == 1, c[3](1, i)[...].astype(F32), 0.0)

    def own_tail(i):
        own_wait(tail_chain, i)
        here = tail_view(0, i)
        here[...] = (here[...].astype(F32) + own_rows(tail_chain, i)).astype(BF16)

    def first_send():
        spread[0][0].start()
        spread[0][1].start()
        line_send(lines)
        on_mid(lambda: line_send_inner(lines))
        for copy in small:
            copy.start()
        spread[0][2].start()
        spread[0][3].start()
        for copy in swap:
            copy.start()

    def make_tables():
        for copy in small:
            copy.wait_recv()
        make_slots()
        for copy in keep:
            copy.wait()

    def swapped():
        for copy in swap:
            copy.wait_recv()

    def run(events):
        n = 0
        while n < len(events):
            who, stop = events[n][0], n + 1
            while stop < len(events) and events[stop][0] == who:
                stop += 1
            group = events[n:stop]

            def do(group=group):
                for event in group:
                    acts[event[1]](*event[2:])

            {"all": lambda f: f(), "end": on_end, "mid": on_mid}[who](do)
            n = stop

    acts = {
        "Start": first_send,
        "T": make_tables,
        "Swap": swapped,
        "Ss": spread_send,
        "Sr": spread_relay,
        "Sd": spread_done,
        "Lr": lambda k, i: line_relay(lines, k, i),
        "Lw": lambda k: line_wait(lines, k),
        "Bs": lambda: line_send(bands),
        "Bi": lambda: line_send_inner(bands),
        "Br": lambda k, i: line_relay(bands, k, i),
        "Bw": lambda k: line_wait(bands, k),
        "C": lambda k, hook: compute(k, lambda: run(hook)),
        "F1": fold_one,
        "F2": fold_two,
        "F3": fold_three,
        "De": lambda k, i: tail_chain[0][k, i].start(),
        "Dm": lambda k, i: chain_mid(tail_chain, k, i),
        "Dw": own_tail,
        "Ce": lambda k, i: rows_chain[0][k, i].start(),
        "Cm": lambda k, i: chain_mid(rows_chain, k, i),
        "Cw": lambda i: own_wait(rows_chain, i),
    }
    run(ORDER)
    for i, piece in enumerate(part_rows):
        out[piece] = (fold_sum(0, i) + own_rows(rows_chain, i)).astype(BF16)

    for group in spread + folds + [small, swap]:
        for copy in group:
            copy.wait_send()
    for i in range(2):
        for copies in (lines, bands):
            copies[i][0].wait_send()
        for c in (rows_chain, tail_chain):
            c[0][1, i].wait_send()

    @pl.when(mid == 1)
    def _():
        for i in range(2):
            for copies in (lines, bands):
                for copy in copies[i][1:]:
                    copy.wait_send()
            for c in (rows_chain, tail_chain):
                c[1][2, i].wait_send()
                c[1][3, i].wait_send()

    @pl.when(mid == 0)
    def _():
        for i in range(2):
            for c in (rows_chain, tail_chain):
                c[0][2, i].wait_send()
                c[0][3, i].wait_send()


def on_layers(levels, tokens, expert_ids, route_weights, w_gate, w_up, w_down):
    tok_rows, width = tokens.shape
    top_count = expert_ids.shape[1]
    device_count = lax.axis_size("side") * levels
    capacity = 2 * tok_rows * top_count // device_count
    chips = device_count // 2
    columns = chips // levels
    spare = tok_rows // 4
    main = tok_rows - spare
    cut = (main // 2 + 15) // 16 * 16
    anywhere = pl.BlockSpec(memory_space=pl.ANY)
    vmem = pltpu.VMEM
    dma = pltpu.SemaphoreType.DMA
    return pl.pallas_call(
        functools.partial(fused_kernel, levels, spare),
        out_shape=jax.ShapeDtypeStruct((tok_rows, width), BF16),
        in_specs=[anywhere] * 6,
        out_specs=pl.BlockSpec(memory_space=vmem),
        scratch_shapes=[
            vmem((top_count, tok_rows), jnp.int32),
            vmem((top_count, tok_rows), F32),
            vmem((chips, 8, tok_rows), F32),
            vmem((chips, 8, tok_rows), F32),
            vmem((chips, 8, tok_rows), F32),
            vmem((2,) + w_gate.shape[1:], BF16),
            vmem((2,) + w_up.shape[1:], BF16),
            vmem((2,) + w_down.shape[1:], BF16),
            vmem((levels, columns, tok_rows, width), BF16),
            vmem((levels, columns, tok_rows, width), BF16),
            vmem((2, columns * capacity, width), BF16),
            vmem((2, columns * capacity, width), BF16),
            vmem((columns, tok_rows, 2 * capacity), BF16),
            vmem((levels + 1, 4, cut, width), BF16),
            vmem((levels + 1, 2, cut, width), BF16),
            vmem((5, main, width), BF16),
            vmem((5, columns, spare, width), BF16),
            dma((levels, 6)),
            dma((levels, 6)),
            dma((5, 2)),
            dma((4, 2)),
            dma((5, 2)),
            dma((4, 2)),
            dma((levels + 1, 6)),
            dma((levels + 1, 6)),
            dma((4, 2)),
            dma((5, 2)),
            dma((4, 2)),
            dma((5, 2)),
            dma((chips - 1,)),
            dma((chips - 1,)),
            dma((3,)),
            dma((3,)),
            dma((6,)),
        ],
        compiler_params=pltpu.CompilerParams(
            collective_id=0, has_side_effects=True, vmem_limit_bytes=62 * 2**20
        ),
        name="layer",
    )(tokens, expert_ids.T, route_weights.T, w_gate, w_up, w_down)


def expert_ffn(rows, gate_proj, up_proj, down_proj):
    gate = jnp.dot(rows, gate_proj, preferred_element_type=jnp.float32)
    upper = jnp.dot(rows, up_proj, preferred_element_type=jnp.float32)
    hidden = (jax.nn.silu(gate) * upper).astype(jnp.bfloat16)
    return jnp.dot(hidden, down_proj, preferred_element_type=jnp.float32).astype(jnp.bfloat16)


def on_device(tokens, expert_ids, route_weights, w_gate, w_up, w_down):
    tok_rows = tokens.shape[0]
    width = tokens.shape[1]
    top_count = expert_ids.shape[1]
    side_count = lax.axis_size("side")
    device_count = side_count * lax.axis_size("lane")
    local_count = w_gate.shape[0]
    expert_count = device_count * local_count
    capacity = 2 * tok_rows * top_count // expert_count
    flat_ids = expert_ids.reshape(-1)
    onehot = (flat_ids[:, None] == jnp.arange(expert_count, dtype=jnp.int32)[None, :]).astype(
        jnp.int32
    )
    earlier = jnp.cumsum(onehot, axis=0) - onehot
    slot_index = jnp.sum(earlier * onehot, axis=1)
    position = (flat_ids * capacity + slot_index).reshape(tok_rows, top_count)
    buffer_rows = jnp.arange(expert_count * capacity, dtype=jnp.int32)
    dispatch_table = jnp.any(buffer_rows[:, None, None] == position[None, :, :], axis=2).astype(
        jnp.bfloat16
    )
    outgoing = jnp.dot(dispatch_table, tokens, preferred_element_type=jnp.float32).astype(
        jnp.bfloat16
    )
    outgoing = outgoing.reshape(expert_count, capacity, width)
    received = lax.all_to_all(outgoing, ("side", "lane"), split_axis=0, concat_axis=0, tiled=True)
    count = received.shape[1]
    grouped = received.reshape(device_count, local_count, count, width)
    rows = grouped[:, 0].reshape(device_count * count, width)
    output = expert_ffn(rows, w_gate[0], w_up[0], w_down[0])
    results = [output.reshape(device_count, count, width)]
    returned = lax.all_to_all(
        jnp.stack(results, axis=1).reshape(device_count * local_count, count, width),
        ("side", "lane"),
        split_axis=0,
        concat_axis=0,
        tiled=True,
    )
    flat_back = returned.reshape(expert_count * capacity, width)
    picked = flat_back[position]
    mixed = jnp.einsum("tk,tkd->td", route_weights, picked, preferred_element_type=jnp.float32)
    return mixed.astype(jnp.bfloat16)


def layered(mesh, tokens):
    side, levels = mesh.shape["side"], mesh.shape["lane"]
    layer_bytes = tokens.shape[0] // 2 * tokens.shape[1] * tokens.dtype.itemsize
    fits = 3 * layer_bytes < 32 * 2**20 and side * levels <= tokens.shape[0] // (side * levels) == 2**7
    return side == 2**3 and levels == 4 and fits


def solution(mesh):
    placed = (
        P(AXES, None),
        P(AXES, None),
        P(AXES, None),
        P(AXES, None, None),
        P(AXES, None, None),
        P(AXES, None, None),
    )

    def run(tokens, *rest):
        body = on_device
        if layered(mesh, tokens):
            body = functools.partial(on_layers, mesh.shape["lane"])
        return jax.shard_map(
            body, mesh=mesh, in_specs=placed, out_specs=P(AXES, None), check_vma=False
        )(tokens, *rest)

    return run
```

```python
import functools

import jax
import jax.numpy as jnp
from jax import lax
from jax.experimental import pallas as pl
from jax.experimental.pallas import tpu as pltpu
from jax.sharding import PartitionSpec as P

AXES = ("side", "lane")
MESH = pl.DeviceIdType.MESH
BF16 = jnp.bfloat16
F32 = jnp.float32


ORDER = [
    ("all", "Start"), ("end", "Sr", 0), ("end", "Lw", 3), ("end", "T"), ("end", "Ss", 3),
    ("end", "Lw", 1), ("end", "Ss", 1), ("end", "Sd", 0), ("end", "Bs"), ("mid", "Sr", 0),
    ("mid", "Lr", 1, 0), ("mid", "Lr", 2, 0), ("mid", "T"), ("mid", "Lr", 2, 1), ("mid", "Ss", 2),
    ("mid", "Lr", 1, 1), ("mid", "Sd", 0), ("mid", "Bi"), ("mid", "Ss", 1), ("mid", "Lr", 3, 0),
    ("all", "C", 0, [
        ("end", "Sr", 1), ("all", "Swap"),
    ]),
    ("end", "Lw", 2), ("end", "Ss", 2), ("end", "Sr", 2), ("end", "Bw", 1), ("end", "Sd", 1),
    ("end", "Sr", 3), ("mid", "Lr", 3, 1), ("mid", "Sr", 1), ("mid", "Sr", 2), ("mid", "Br", 2, 0),
    ("mid", "Br", 1, 0), ("mid", "Br", 2, 1), ("mid", "Ss", 3), ("mid", "Sd", 1), ("mid", "Br", 3, 0),
    ("mid", "Br", 1, 1),
    ("all", "C", 1, [
    ]),
    ("end", "De", 1, 1), ("end", "Bw", 2), ("end", "Sd", 2), ("end", "De", 1, 0), ("end", "F1", 1),
    ("mid", "Sd", 2), ("mid", "Br", 3, 1), ("mid", "Sr", 3), ("mid", "F1", 1),
    ("all", "C", 2, [
        ("end", "Sd", 3),
    ]),
    ("end", "F1", 2), ("end", "De", 2, 0), ("end", "De", 2, 1), ("end", "F2", 1), ("end", "Bw", 3),
    ("mid", "Bs"), ("mid", "Sd", 3),
    ("all", "C", 3, [
        ("mid", "Dm", 2, 1), ("mid", "F1", 2), ("mid", "Dm", 2, 0), ("mid", "F2", 1),
    ]),
    ("end", "De", 3, 0), ("end", "F2", 2), ("end", "F1", 3), ("end", "De", 3, 1), ("end", "F3", 2, 0),
    ("end", "Ce", 2, 0), ("end", "F3", 2, 1), ("end", "Ce", 2, 1), ("end", "F2", 3), ("end", "F1", 0),
    ("end", "F3", 1, 0), ("end", "Ce", 1, 0), ("end", "F3", 1, 1), ("end", "F3", 3, 1),
    ("end", "Dw", 0), ("end", "Ce", 1, 1), ("end", "F3", 3, 0), ("end", "Ce", 3, 1), ("end", "Dw", 1),
    ("end", "F1", 4), ("end", "F2", 0), ("end", "Ce", 3, 0), ("end", "F2", 4), ("end", "Cw", 1),
    ("end", "F3", 4, 1), ("end", "Cw", 0), ("end", "F3", 4, 0), ("end", "F3", 0, 0),
    ("end", "F3", 0, 1), ("mid", "F1", 3), ("mid", "Dm", 3, 0), ("mid", "Dm", 3, 1),
    ("mid", "Dm", 1, 0), ("mid", "F3", 1, 1), ("mid", "F2", 3), ("mid", "F2", 2), ("mid", "F3", 3, 0),
    ("mid", "Cm", 3, 0), ("mid", "F3", 3, 1), ("mid", "Dw", 1), ("mid", "Dm", 1, 1), ("mid", "Dw", 0),
    ("mid", "F1", 0), ("mid", "Cm", 3, 1), ("mid", "F3", 2, 1), ("mid", "F3", 1, 0), ("mid", "F1", 4),
    ("mid", "F3", 2, 0), ("mid", "Cm", 1, 0), ("mid", "F2", 0), ("mid", "Cm", 2, 0),
    ("mid", "Cm", 2, 1), ("mid", "Cm", 1, 1), ("mid", "F2", 4), ("mid", "Cw", 1), ("mid", "F3", 0, 0),
    ("mid", "F3", 0, 1), ("mid", "F3", 4, 1), ("mid", "F3", 4, 0), ("mid", "Cw", 0),
]


def flip(value, mask):
    bit = 1
    out = value
    while bit <= mask:
        if mask & bit:
            out = out + bit - 2 * bit * ((value // bit) % 2)
        bit *= 2
    return out


def fused_kernel(
    levels, spare, tokens, ids, gains, wg, wu, wd, out, ids_v, gains_v, mine, shares, slots, wgs, wus, wds, every,
    part, xs, ys, backs, first, second, row_in, plane_in, gs, gr, zs, zr, bs, br, ps, pr, cs, cr, ds, dr, ss, sr, ws,
    wr, local
):
    side, level = lax.axis_index("side"), lax.axis_index("lane")
    col, core = side // 2, side % 2
    mid = ((level + 1) // 2) % 2
    rows = out.shape[0]
    width = out.shape[1]
    chips = shares.shape[0]
    columns = chips // levels
    cap = xs.shape[1] // columns
    main = rows - spare
    cut = (main // 2 + 7) // 8 * 8
    bcut = (spare // 2 + 7) // 8 * 8
    whole = (pl.ds(0, rows // 2), pl.ds(rows // 2, rows // 2))
    part_rows = (pl.ds(0, cut), pl.ds(cut, main - cut))
    tail_rows = (pl.ds(main, bcut), pl.ds(main + bcut, spare - bcut))
    dev_x, dev_y = (flip(col, 1) * 2 + core, level), (flip(col, 2) * 2 + core, level)
    twin = (col * 2 + 1 - core, level)
    mate = (side, flip(level, 1))
    inner = (side, mid * flip(level, 3) + (1 - mid) * flip(level, 1))
    lev = [
        level,
        mid * flip(level, 1) + (1 - mid) * flip(level, 2),
        flip(level, 3),
        mid * flip(level, 2) + (1 - mid) * flip(level, 1),
    ]
    me = col * levels + level
    others = [(flip(col, m // levels), flip(level, m % levels)) for m in range(1, chips)]

    fetch = [pltpu.make_async_copy(ids, ids_v, local.at[0]), pltpu.make_async_copy(gains, gains_v, local.at[1])]
    for copy in fetch:
        copy.start()
    barrier = pltpu.get_barrier_semaphore()
    friends = [(q * 2 + core, z) for q, z in others] + [twin]
    for device in friends:
        pl.semaphore_signal(barrier, inc=1, device_id=device, device_id_type=MESH)
    keep = [
        pltpu.make_async_copy(tokens, every.at[0, 0], local.at[2]),
        pltpu.make_async_copy(wg.at[0], wgs.at[0], local.at[3]),
        pltpu.make_async_copy(wu.at[0], wus.at[0], local.at[4]),
        pltpu.make_async_copy(wd.at[0], wds.at[0], local.at[5]),
    ]
    for copy in keep:
        copy.start()
    for copy in fetch:
        copy.wait()
    number = lax.broadcasted_iota(jnp.int32, (2 * chips, rows), 0)
    table = jnp.zeros((2 * chips, rows), F32)
    for k in range(ids_v.shape[0]):
        table = table + jnp.where(ids_v[k : k + 1] == number, gains_v[k : k + 1], 0.0)
    for q in range(columns):
        for z in range(levels):
            for c in range(2):
                e = (q * 2 + c) * levels + z
                mine[q * levels + z, c : c + 1, :] = table[e : e + 1, :]
            mine[q * levels + z, 2:8, :] = jnp.zeros((6, rows), F32)
    shares[me] = mine[me]
    pl.semaphore_wait(barrier, len(friends))

    def link(src, dst, s, r, device):
        return pltpu.make_async_remote_copy(
            src_ref=src, dst_ref=dst, send_sem=s, recv_sem=r, device_id=device, device_id_type=MESH
        )

    def on_mid(do):
        pl.when(mid == 1)(do)

    def on_end(do):
        pl.when(mid == 0)(do)

    def spread_copies(k):
        p, q = whole if k == 0 else part_rows
        block = tokens if k == 0 else every.at[k, 0]
        return [
            link(block.at[p], every.at[k, 1, p], gs.at[k, 0], gr.at[k, 0], dev_x),
            link(block.at[q], every.at[k, 2, q], gs.at[k, 1], gr.at[k, 1], dev_y),
            link(block.at[q], every.at[k, 1, q], gs.at[k, 2], gr.at[k, 2], dev_x),
            link(block.at[p], every.at[k, 2, p], gs.at[k, 3], gr.at[k, 3], dev_y),
            link(every.at[k, 1, p], every.at[k, 3, p], gs.at[k, 4], gr.at[k, 4], dev_y),
            link(every.at[k, 2, q], every.at[k, 3, q], gs.at[k, 5], gr.at[k, 5], dev_x),
        ]

    spread = [spread_copies(k) for k in range(levels)]

    def spread_send(k):
        for i in range(4):
            spread[k][i].start()

    def spread_relay(k):
        spread[k][0].wait_recv()
        spread[k][4].start()
        spread[k][1].wait_recv()
        spread[k][5].start()

    def spread_done(k):
        for i in range(2, 6):
            spread[k][i].wait_recv()

    there = 1 + 2 * mid
    def line_copies(view, own, s, r):
        out = []
        for i in range(2):
            out.append(
                [
                    link(own(i), view(there, i), s.at[0, i], r.at[there, i], mate),
                    link(own(i), view(2, i), s.at[1, i], r.at[2, i], inner),
                    link(view(1, i), view(3, i), s.at[2, i], r.at[3, i], inner),
                    link(view(2, i), view(1, i), s.at[3, i], r.at[1, i], mate),
                    link(view(3, i), view(2, i), s.at[4, i], r.at[2, i], mate),
                    link(view(1, i), view(1, i), s.at[0, i], r.at[1, i], mate),
                    link(view(2, i), view(2, i), s.at[0, i], r.at[2, i], mate),
                    link(view(3, i), view(3, i), s.at[0, i], r.at[3, i], mate),
                ]
            )
        return out

    block_rows = (pl.ds(0, cut), pl.ds(cut, rows - cut))
    lines = line_copies(
        lambda k, i: every.at[k, 0, block_rows[i]], lambda i: tokens.at[block_rows[i]], zs, zr
    )

    def tails(k, i):
        return every.at[k, pl.ds(1, columns - 1), tail_rows[i]]

    bands = line_copies(tails, lambda i: tails(0, i), bs, br)

    def line_send(copies):
        for i in range(2):
            copies[i][0].start()

    def line_send_inner(copies):
        for i in range(2):
            copies[i][1].start()

    def line_wait(copies, k):
        for i in range(2):
            copies[i][k + 4].wait_recv()

    def line_relay(copies, k, i):
        copies[i][k + 4].wait_recv()
        copies[i][k + 1].start()

    small = [
        link(mine.at[q * levels + z], shares.at[me], ss.at[i], sr.at[i], (q * 2 + core, z))
        for i, (q, z) in enumerate(others)
    ]
    swap = [
        link(wg.at[0], wgs.at[1], ws.at[0], wr.at[0], twin),
        link(wu.at[0], wus.at[1], ws.at[1], wr.at[1], twin),
        link(wd.at[0], wds.at[1], ws.at[2], wr.at[2], twin),
    ]

    def make_slots():
        chosen = (shares[...] > 0.0).astype(F32).astype(BF16).reshape(chips * 8, rows)
        before = lax.broadcasted_iota(jnp.int32, (rows, rows), 0) < lax.broadcasted_iota(
            jnp.int32, (rows, rows), 1
        )
        before = before.astype(F32).astype(BF16)
        slots[...] = jnp.dot(chosen, before, preferred_element_type=F32).reshape(chips, 8, rows)

    def compute(k, middle):
        place = lax.broadcasted_iota(jnp.int32, (cap, rows), 0).astype(F32)

        def pick(r, carry):
            b = (((col // 2 + r // 2) % 2) * 2 + (col + r) % 2) * levels + lev[k]
            gain, slot = shares[b], slots[b]
            wanted = []
            for e in range(2):
                g = jnp.where(core == 0, gain[e : e + 1], gain[1 - e : 2 - e])
                s = jnp.where(core == 0, slot[e : e + 1], slot[1 - e : 2 - e])
                wanted.append(jnp.where(s == place, g, 0.0))
            weights = jnp.concatenate(wanted, axis=0)
            chosen = jnp.where(weights > 0.0, 1.0, 0.0).astype(BF16)
            backs[r] = weights.T.astype(BF16)
            picked = jnp.dot(chosen, every[k, r], preferred_element_type=F32).astype(BF16)
            at = pl.ds(pl.multiple_of(r * cap, cap), cap)
            for e in range(2):
                xs[e, at] = picked[e * cap : (e + 1) * cap]
            return carry

        lax.fori_loop(0, columns, pick, 0)

        def expert(e, carry):
            @pl.when(e == 1)
            def _():
                middle()

            x = xs[e]
            gate = jnp.dot(x, wgs[e], preferred_element_type=F32)
            upper = jnp.dot(x, wus[e], preferred_element_type=F32)
            hidden = (gate / (1.0 + jnp.exp(-gate)) * upper).astype(BF16)
            ys[e] = jnp.dot(hidden, wds[e], preferred_element_type=F32).astype(BF16)
            return carry

        lax.fori_loop(0, 2, expert, 0)

        def mix(r, carry):
            at = pl.ds(pl.multiple_of(r * cap, cap), cap)
            y = jnp.concatenate([ys[e, at] for e in range(2)], axis=0)
            part[k, r] = jnp.dot(backs[r], y, preferred_element_type=F32).astype(BF16)
            return carry

        lax.fori_loop(0, columns, mix, 0)

    def fold_copies(g):
        k = g % levels
        p, q = part_rows if g < levels else tail_rows
        a, b = pl.ds(0, p.size), pl.ds(0, q.size)
        return [
            link(part.at[k, 3, p], first.at[g, 0, a], ps.at[g, 0], pr.at[g, 0], dev_x),
            link(part.at[k, 3, q], first.at[g, 1, b], ps.at[g, 1], pr.at[g, 1], dev_y),
            link(part.at[k, 1, p], first.at[g, 2, a], ps.at[g, 2], pr.at[g, 2], dev_x),
            link(part.at[k, 2, q], first.at[g, 3, b], ps.at[g, 3], pr.at[g, 3], dev_y),
            link(part.at[k, 2, p], second.at[g, 0, a], ps.at[g, 4], pr.at[g, 4], dev_y),
            link(part.at[k, 1, q], second.at[g, 1, b], ps.at[g, 5], pr.at[g, 5], dev_x),
        ]

    folds = [fold_copies(g) for g in range(levels + 1)]

    def fold_one(g):
        for i in range(4):
            folds[g][i].start()

    def fold_two(g):
        k = g % levels
        p, q = part_rows if g < levels else tail_rows
        for i, (r, piece) in enumerate(((2, p), (1, q))):
            folds[g][i].wait_recv()
            part[k, r, piece] = (
                part[k, r, piece].astype(F32) + first[g, i, pl.ds(0, piece.size)].astype(F32)
            ).astype(BF16)
            folds[g][4 + i].start()

    def fold_wait(g, i):
        folds[g][2 + i].wait_recv()
        folds[g][4 + i].wait_recv()

    def fold_sum(g, i):
        k = g % levels
        piece = (part_rows if g < levels else tail_rows)[i]
        at = pl.ds(0, piece.size)
        return (
            part[k, 0, piece].astype(F32) + first[g, 2 + i, at].astype(F32) + second[g, i, at].astype(F32)
        )

    def fold_three(g, i):
        fold_wait(g, i)
        if g == levels:
            out[tail_rows[i]] = fold_sum(g, i).astype(BF16)
        elif g:
            part[g, 0, part_rows[i]] = fold_sum(g, i).astype(BF16)

    def chain(view, land, s, r):
        send_end, send_mid = {}, {}
        for i in range(2):
            for k, end_slot, mid_slot in ((3, 0, 4), (2, 3, 1), (1, 2, 0)):
                send_end[k, i] = link(view(k, i), land(end_slot, i), s.at[k, i], r.at[end_slot, i], mate)
                send_mid[k, i] = link(
                    view(k, i), land(mid_slot, i), s.at[k, i], r.at[mid_slot, i], mate if k == 1 else inner
                )
        return send_end, send_mid, view, land, r

    def main_view(k, i):
        return part.at[k, 0, part_rows[i]]

    def tail_view(k, i):
        return part.at[k, pl.ds(0, columns), tail_rows[i]]

    rows_chain = chain(main_view, lambda slot, i: row_in.at[slot, part_rows[i]], cs, cr)
    tail_chain = chain(
        tail_view,
        lambda slot, i: plane_in.at[slot, pl.ds(0, columns), (pl.ds(0, bcut), pl.ds(bcut, spare - bcut))[i]],
        ds,
        dr,
    )

    def landed(c, slot, i):
        land, r = c[3], c[4]
        link(land(slot, i), land(slot, i), r.at[slot, i], r.at[slot, i], mate).wait_recv()

    def chain_mid(c, k, i):
        slot = {3: 3, 2: 2, 1: 4}[k]
        landed(c, slot, i)
        here = c[2](k, i)
        here[...] = (here[...].astype(F32) + c[3](slot, i)[...].astype(F32)).astype(BF16)
        c[1][k, i].start()

    def own_wait(c, i):
        landed(c, 0, i)

        @pl.when(mid == 1)
        def _():
            landed(c, 1, i)

    def own_rows(c, i):
        return c[3](0, i)[...].astype(F32) + jnp.where(mid == 1, c[3](1, i)[...].astype(F32), 0.0)

    def own_tail(i):
        own_wait(tail_chain, i)
        here = tail_view(0, i)
        here[...] = (here[...].astype(F32) + own_rows(tail_chain, i)).astype(BF16)

    def first_send():
        spread[0][0].start()
        spread[0][1].start()
        line_send(lines)
        on_mid(lambda: line_send_inner(lines))
        for copy in small:
            copy.start()
        spread[0][2].start()
        spread[0][3].start()
        for copy in swap:
            copy.start()

    def make_tables():
        for copy in small:
            copy.wait_recv()
        make_slots()
        for copy in keep:
            copy.wait()

    def swapped():
        for copy in swap:
            copy.wait_recv()

    def run(events):
        n = 0
        while n < len(events):
            who, stop = events[n][0], n + 1
            while stop < len(events) and events[stop][0] == who:
                stop += 1
            group = events[n:stop]

            def do(group=group):
                for event in group:
                    acts[event[1]](*event[2:])

            {"all": lambda f: f(), "end": on_end, "mid": on_mid}[who](do)
            n = stop

    acts = {
        "Start": first_send,
        "T": make_tables,
        "Swap": swapped,
        "Ss": spread_send,
        "Sr": spread_relay,
        "Sd": spread_done,
        "Lr": lambda k, i: line_relay(lines, k, i),
        "Lw": lambda k: line_wait(lines, k),
        "Bs": lambda: line_send(bands),
        "Bi": lambda: line_send_inner(bands),
        "Br": lambda k, i: line_relay(bands, k, i),
        "Bw": lambda k: line_wait(bands, k),
        "C": lambda k, hook: compute(k, lambda: run(hook)),
        "F1": fold_one,
        "F2": fold_two,
        "F3": fold_three,
        "De": lambda k, i: tail_chain[0][k, i].start(),
        "Dm": lambda k, i: chain_mid(tail_chain, k, i),
        "Dw": own_tail,
        "Ce": lambda k, i: rows_chain[0][k, i].start(),
        "Cm": lambda k, i: chain_mid(rows_chain, k, i),
        "Cw": lambda i: own_wait(rows_chain, i),
    }
    run(ORDER)
    for i, piece in enumerate(part_rows):
        out[piece] = (fold_sum(0, i) + own_rows(rows_chain, i)).astype(BF16)

    for group in spread + folds + [small, swap]:
        for copy in group:
            copy.wait_send()
    for i in range(2):
        for copies in (lines, bands):
            copies[i][0].wait_send()
        for c in (rows_chain, tail_chain):
            c[0][1, i].wait_send()
            c[0][2, i].wait_send()
            c[0][3, i].wait_send()

    @pl.when(mid == 1)
    def _():
        for i in range(2):
            for copies in (lines, bands):
                for copy in copies[i][1:5]:
                    copy.wait_send()


def on_layers(levels, tokens, expert_ids, route_weights, w_gate, w_up, w_down):
    tok_rows, width = tokens.shape
    top_count = expert_ids.shape[1]
    device_count = lax.axis_size("side") * levels
    capacity = 2 * tok_rows * top_count // device_count
    chips = device_count // 2
    columns = chips // levels
    spare = tok_rows // 4
    main = tok_rows - spare
    cut = (main // 2 + 7) // 8 * 8
    anywhere = pl.BlockSpec(memory_space=pl.ANY)
    vmem = pltpu.VMEM
    dma = pltpu.SemaphoreType.DMA
    return pl.pallas_call(
        functools.partial(fused_kernel, levels, spare),
        out_shape=jax.ShapeDtypeStruct((tok_rows, width), BF16),
        in_specs=[anywhere] * 6,
        out_specs=pl.BlockSpec(memory_space=vmem),
        scratch_shapes=[
            vmem((top_count, tok_rows), jnp.int32),
            vmem((top_count, tok_rows), F32),
            vmem((chips, 8, tok_rows), F32),
            vmem((chips, 8, tok_rows), F32),
            vmem((chips, 8, tok_rows), F32),
            vmem((2,) + w_gate.shape[1:], BF16),
            vmem((2,) + w_up.shape[1:], BF16),
            vmem((2,) + w_down.shape[1:], BF16),
            vmem((levels, columns, tok_rows, width), BF16),
            vmem((levels, columns, tok_rows, width), BF16),
            vmem((2, columns * capacity, width), BF16),
            vmem((2, columns * capacity, width), BF16),
            vmem((columns, tok_rows, 2 * capacity), BF16),
            vmem((levels + 1, 4, cut, width), BF16),
            vmem((levels + 1, 2, cut, width), BF16),
            vmem((5, main, width), BF16),
            vmem((5, columns, spare, width), BF16),
            dma((levels, 6)),
            dma((levels, 6)),
            dma((5, 2)),
            dma((4, 2)),
            dma((5, 2)),
            dma((4, 2)),
            dma((levels + 1, 6)),
            dma((levels + 1, 6)),
            dma((4, 2)),
            dma((5, 2)),
            dma((4, 2)),
            dma((5, 2)),
            dma((chips - 1,)),
            dma((chips - 1,)),
            dma((3,)),
            dma((3,)),
            dma((6,)),
        ],
        compiler_params=pltpu.CompilerParams(
            collective_id=0, has_side_effects=True, vmem_limit_bytes=62 * 2**20
        ),
        name="layer",
    )(tokens, expert_ids.T, route_weights.T, w_gate, w_up, w_down)


def expert_ffn(rows, gate_proj, up_proj, down_proj):
    gate = jnp.dot(rows, gate_proj, preferred_element_type=jnp.float32)
    upper = jnp.dot(rows, up_proj, preferred_element_type=jnp.float32)
    hidden = (jax.nn.silu(gate) * upper).astype(jnp.bfloat16)
    return jnp.dot(hidden, down_proj, preferred_element_type=jnp.float32).astype(jnp.bfloat16)


def on_device(tokens, expert_ids, route_weights, w_gate, w_up, w_down):
    tok_rows = tokens.shape[0]
    width = tokens.shape[1]
    top_count = expert_ids.shape[1]
    side_count = lax.axis_size("side")
    device_count = side_count * lax.axis_size("lane")
    local_count = w_gate.shape[0]
    expert_count = device_count * local_count
    capacity = 2 * tok_rows * top_count // expert_count
    flat_ids = expert_ids.reshape(-1)
    onehot = (flat_ids[:, None] == jnp.arange(expert_count, dtype=jnp.int32)[None, :]).astype(
        jnp.int32
    )
    earlier = jnp.cumsum(onehot, axis=0) - onehot
    slot_index = jnp.sum(earlier * onehot, axis=1)
    position = (flat_ids * capacity + slot_index).reshape(tok_rows, top_count)
    buffer_rows = jnp.arange(expert_count * capacity, dtype=jnp.int32)
    dispatch_table = jnp.any(buffer_rows[:, None, None] == position[None, :, :], axis=2).astype(
        jnp.bfloat16
    )
    outgoing = jnp.dot(dispatch_table, tokens, preferred_element_type=jnp.float32).astype(
        jnp.bfloat16
    )
    outgoing = outgoing.reshape(expert_count, capacity, width)
    received = lax.all_to_all(outgoing, ("side", "lane"), split_axis=0, concat_axis=0, tiled=True)
    count = received.shape[1]
    grouped = received.reshape(device_count, local_count, count, width)
    rows = grouped[:, 0].reshape(device_count * count, width)
    output = expert_ffn(rows, w_gate[0], w_up[0], w_down[0])
    results = [output.reshape(device_count, count, width)]
    returned = lax.all_to_all(
        jnp.stack(results, axis=1).reshape(device_count * local_count, count, width),
        ("side", "lane"),
        split_axis=0,
        concat_axis=0,
        tiled=True,
    )
    flat_back = returned.reshape(expert_count * capacity, width)
    picked = flat_back[position]
    mixed = jnp.einsum("tk,tkd->td", route_weights, picked, preferred_element_type=jnp.float32)
    return mixed.astype(jnp.bfloat16)


def layered(mesh, tokens):
    side, levels = mesh.shape["side"], mesh.shape["lane"]
    layer_bytes = tokens.shape[0] // 2 * tokens.shape[1] * tokens.dtype.itemsize
    fits = 3 * layer_bytes < 32 * 2**20 and side * levels <= tokens.shape[0] // (side * levels) == 2**7
    return side == 2**3 and levels == 4 and fits


def solution(mesh):
    placed = (
        P(AXES, None),
        P(AXES, None),
        P(AXES, None),
        P(AXES, None, None),
        P(AXES, None, None),
        P(AXES, None, None),
    )

    def run(tokens, *rest):
        body = on_device
        if layered(mesh, tokens):
            body = functools.partial(on_layers, mesh.shape["lane"])
        return jax.shard_map(
            body, mesh=mesh, in_specs=placed, out_specs=P(AXES, None), check_vma=False
        )(tokens, *rest)

    return run
```

```python
import functools

import jax
import jax.numpy as jnp
from jax import lax
from jax.experimental import pallas as pl
from jax.experimental.pallas import tpu as pltpu
from jax.sharding import PartitionSpec as P

AXES = ("side", "lane")
MESH = pl.DeviceIdType.MESH
BF16 = jnp.bfloat16
F32 = jnp.float32


ORDER = [
    ("all", "Start"), ("end", "Sr", 0), ("end", "Lw", 3), ("end", "T"), ("end", "Ss", 3),
    ("end", "Lw", 1), ("end", "Ss", 1), ("end", "Sd", 0), ("end", "Bs"), ("mid", "Sr", 0),
    ("mid", "Lr", 1, 0), ("mid", "Lr", 2, 0), ("mid", "T"), ("mid", "Lr", 2, 1), ("mid", "Ss", 2),
    ("mid", "Lr", 1, 1), ("mid", "Sd", 0), ("mid", "Bi"), ("mid", "Ss", 1), ("mid", "Lr", 3, 0),
    ("all", "C", 0, [
        ("end", "Sr", 1), ("all", "Swap"),
    ]),
    ("end", "Lw", 2), ("end", "Ss", 2), ("end", "Sr", 2), ("end", "Bw", 1), ("end", "Sd", 1),
    ("end", "Sr", 3), ("mid", "Lr", 3, 1), ("mid", "Sr", 1), ("mid", "Sr", 2), ("mid", "Br", 2, 0),
    ("mid", "Br", 1, 0), ("mid", "Br", 2, 1), ("mid", "Ss", 3), ("mid", "Sd", 1), ("mid", "Br", 3, 0),
    ("mid", "Br", 1, 1),
    ("all", "C", 1, [
    ]),
    ("end", "De", 1, 1), ("end", "Bw", 2), ("end", "Sd", 2), ("end", "De", 1, 0), ("end", "F1", 1),
    ("mid", "Sd", 2), ("mid", "Br", 3, 1), ("mid", "Sr", 3), ("mid", "F1", 1),
    ("all", "C", 2, [
        ("end", "Sd", 3),
    ]),
    ("end", "F1", 2), ("end", "De", 2, 0), ("end", "De", 2, 1), ("end", "F2", 1), ("end", "Bw", 3),
    ("mid", "Bs"), ("mid", "Sd", 3),
    ("all", "C", 3, [
        ("mid", "Dm", 2, 1), ("mid", "F1", 2), ("mid", "Dm", 2, 0), ("mid", "F2", 1),
    ]),
    ("end", "De", 3, 0), ("end", "F2", 2), ("end", "F1", 3), ("end", "De", 3, 1), ("end", "F3", 2, 0),
    ("end", "Ce", 2, 0), ("end", "F3", 2, 1), ("end", "Ce", 2, 1), ("end", "F2", 3), ("end", "F1", 0),
    ("end", "F3", 1, 0), ("end", "Ce", 1, 0), ("end", "F3", 1, 1), ("end", "F3", 3, 1),
    ("end", "Dw", 0), ("end", "Ce", 1, 1), ("end", "F3", 3, 0), ("end", "Ce", 3, 1), ("end", "Dw", 1),
    ("end", "F1", 4), ("end", "F2", 0), ("end", "Ce", 3, 0), ("end", "F2", 4), ("end", "Cw", 1),
    ("end", "F3", 4, 1), ("end", "Cw", 0), ("end", "F3", 4, 0), ("end", "F3", 0, 0),
    ("end", "F3", 0, 1), ("mid", "F1", 3), ("mid", "Dm", 3, 0), ("mid", "Dm", 3, 1),
    ("mid", "Dm", 1, 0), ("mid", "F3", 1, 1), ("mid", "F2", 3), ("mid", "F2", 2), ("mid", "F3", 3, 0),
    ("mid", "Cm", 3, 0), ("mid", "F3", 3, 1), ("mid", "Dw", 1), ("mid", "Dm", 1, 1), ("mid", "Dw", 0),
    ("mid", "F1", 0), ("mid", "Cm", 3, 1), ("mid", "F3", 2, 1), ("mid", "F3", 1, 0), ("mid", "F1", 4),
    ("mid", "F3", 2, 0), ("mid", "Cm", 1, 0), ("mid", "F2", 0), ("mid", "Cm", 2, 0),
    ("mid", "Cm", 2, 1), ("mid", "Cm", 1, 1), ("mid", "F2", 4), ("mid", "Cw", 1), ("mid", "F3", 0, 0),
    ("mid", "F3", 0, 1), ("mid", "F3", 4, 1), ("mid", "F3", 4, 0), ("mid", "Cw", 0),
]


def flip(value, mask):
    bit = 1
    out = value
    while bit <= mask:
        if mask & bit:
            out = out + bit - 2 * bit * ((value // bit) % 2)
        bit *= 2
    return out


def fused_kernel(
    levels, spare, tokens, ids, gains, wg, wu, wd, out, ids_v, gains_v, mine, shares, slots, wgs, wus, wds, every,
    part, xs, ys, backs, first, second, row_in, plane_in, gs, gr, zs, zr, bs, br, ps, pr, cs, cr, ds, dr, ss, sr, ws,
    wr, known, local
):
    side, level = lax.axis_index("side"), lax.axis_index("lane")
    col, core = side // 2, side % 2
    mid = ((level + 1) // 2) % 2
    rows = out.shape[0]
    width = out.shape[1]
    chips = shares.shape[0]
    columns = chips // levels
    cap = xs.shape[1] // columns
    main = rows - spare
    cut = (main // 2 + 7) // 8 * 8
    bcut = (spare // 2 + 7) // 8 * 8
    whole = (pl.ds(0, rows // 2), pl.ds(rows // 2, rows // 2))
    part_rows = (pl.ds(0, cut), pl.ds(cut, main - cut))
    tail_rows = (pl.ds(main, bcut), pl.ds(main + bcut, spare - bcut))
    dev_x, dev_y = (flip(col, 1) * 2 + core, level), (flip(col, 2) * 2 + core, level)
    twin = (col * 2 + 1 - core, level)
    mate = (side, flip(level, 1))
    inner = (side, mid * flip(level, 3) + (1 - mid) * flip(level, 1))
    lev = [
        level,
        mid * flip(level, 1) + (1 - mid) * flip(level, 2),
        flip(level, 3),
        mid * flip(level, 2) + (1 - mid) * flip(level, 1),
    ]
    me = col * levels + level
    others = [(flip(col, m // levels), flip(level, m % levels)) for m in range(1, chips)]

    def on_mid(do):
        pl.when(mid == 1)(do)

    def on_end(do):
        pl.when(mid == 0)(do)

    def tell(sem, device):
        pl.semaphore_signal(sem, inc=1, device_id=device, device_id_type=MESH)

    barrier = pltpu.get_barrier_semaphore()
    for device in (dev_x, dev_y, mate, twin):
        tell(barrier, device)
    on_mid(lambda: tell(barrier, inner))
    fetch = [pltpu.make_async_copy(ids, ids_v, local.at[0]), pltpu.make_async_copy(gains, gains_v, local.at[1])]
    keep = [
        pltpu.make_async_copy(tokens, every.at[0, 0], local.at[2]),
        pltpu.make_async_copy(wg.at[0], wgs.at[0], local.at[3]),
        pltpu.make_async_copy(wu.at[0], wus.at[0], local.at[4]),
        pltpu.make_async_copy(wd.at[0], wds.at[0], local.at[5]),
    ]
    for copy in fetch + keep:
        copy.start()
    pl.semaphore_wait(barrier, 4 + mid)

    def make_mine():
        for copy in fetch:
            copy.wait()
        number = lax.broadcasted_iota(jnp.int32, (2 * chips, rows), 0)
        table = jnp.zeros((2 * chips, rows), F32)
        for k in range(ids_v.shape[0]):
            table = table + jnp.where(ids_v[k : k + 1] == number, gains_v[k : k + 1], 0.0)
        for q in range(columns):
            for z in range(levels):
                for c in range(2):
                    e = (q * 2 + c) * levels + z
                    mine[q * levels + z, c : c + 1, :] = table[e : e + 1, :]
                mine[q * levels + z, 2:8, :] = jnp.zeros((6, rows), F32)
        shares[me] = mine[me]

    def hear_all():
        for device in (dev_x, dev_y):
            tell(known.at[0], device)
        pl.semaphore_wait(known.at[0], 2)
        tell(known.at[1], mate)
        on_mid(lambda: tell(known.at[1], inner))
        pl.semaphore_wait(known.at[1], 1 + mid)

        @pl.when(mid == 1)
        def _():
            tell(known.at[2], mate)
            tell(known.at[2], inner)

        pl.semaphore_wait(known.at[2], 1)
        on_mid(lambda: tell(known.at[3], mate))
        on_end(lambda: pl.semaphore_wait(known.at[3], 1))

    def link(src, dst, s, r, device):
        return pltpu.make_async_remote_copy(
            src_ref=src, dst_ref=dst, send_sem=s, recv_sem=r, device_id=device, device_id_type=MESH
        )

    def spread_copies(k):
        p, q = whole if k == 0 else part_rows
        block = tokens if k == 0 else every.at[k, 0]
        return [
            link(block.at[p], every.at[k, 1, p], gs.at[k, 0], gr.at[k, 0], dev_x),
            link(block.at[q], every.at[k, 2, q], gs.at[k, 1], gr.at[k, 1], dev_y),
            link(block.at[q], every.at[k, 1, q], gs.at[k, 2], gr.at[k, 2], dev_x),
            link(block.at[p], every.at[k, 2, p], gs.at[k, 3], gr.at[k, 3], dev_y),
            link(every.at[k, 1, p], every.at[k, 3, p], gs.at[k, 4], gr.at[k, 4], dev_y),
            link(every.at[k, 2, q], every.at[k, 3, q], gs.at[k, 5], gr.at[k, 5], dev_x),
        ]

    spread = [spread_copies(k) for k in range(levels)]

    def spread_send(k):
        for i in range(4):
            spread[k][i].start()

    def spread_relay(k):
        spread[k][0].wait_recv()
        spread[k][4].start()
        spread[k][1].wait_recv()
        spread[k][5].start()

    def spread_done(k):
        for i in range(2, 6):
            spread[k][i].wait_recv()

    there = 1 + 2 * mid
    def line_copies(view, own, s, r):
        out = []
        for i in range(2):
            out.append(
                [
                    link(own(i), view(there, i), s.at[0, i], r.at[there, i], mate),
                    link(own(i), view(2, i), s.at[1, i], r.at[2, i], inner),
                    link(view(1, i), view(3, i), s.at[2, i], r.at[3, i], inner),
                    link(view(2, i), view(1, i), s.at[3, i], r.at[1, i], mate),
                    link(view(3, i), view(2, i), s.at[4, i], r.at[2, i], mate),
                    link(view(1, i), view(1, i), s.at[0, i], r.at[1, i], mate),
                    link(view(2, i), view(2, i), s.at[0, i], r.at[2, i], mate),
                    link(view(3, i), view(3, i), s.at[0, i], r.at[3, i], mate),
                ]
            )
        return out

    block_rows = (pl.ds(0, cut), pl.ds(cut, rows - cut))
    lines = line_copies(
        lambda k, i: every.at[k, 0, block_rows[i]], lambda i: tokens.at[block_rows[i]], zs, zr
    )

    def tails(k, i):
        return every.at[k, pl.ds(1, columns - 1), tail_rows[i]]

    bands = line_copies(tails, lambda i: tails(0, i), bs, br)

    def line_send(copies):
        for i in range(2):
            copies[i][0].start()

    def line_send_inner(copies):
        for i in range(2):
            copies[i][1].start()

    def line_wait(copies, k):
        for i in range(2):
            copies[i][k + 4].wait_recv()

    def line_relay(copies, k, i):
        copies[i][k + 4].wait_recv()
        copies[i][k + 1].start()

    small = [
        link(mine.at[q * levels + z], shares.at[me], ss.at[i], sr.at[i], (q * 2 + core, z))
        for i, (q, z) in enumerate(others)
    ]
    swap = [
        link(wg.at[0], wgs.at[1], ws.at[0], wr.at[0], twin),
        link(wu.at[0], wus.at[1], ws.at[1], wr.at[1], twin),
        link(wd.at[0], wds.at[1], ws.at[2], wr.at[2], twin),
    ]

    def make_slots():
        chosen = (shares[...] > 0.0).astype(F32).astype(BF16).reshape(chips * 8, rows)
        before = lax.broadcasted_iota(jnp.int32, (rows, rows), 0) < lax.broadcasted_iota(
            jnp.int32, (rows, rows), 1
        )
        before = before.astype(F32).astype(BF16)
        slots[...] = jnp.dot(chosen, before, preferred_element_type=F32).reshape(chips, 8, rows)

    def compute(k, middle):
        place = lax.broadcasted_iota(jnp.int32, (cap, rows), 0).astype(F32)

        def pick(r, carry):
            b = (((col // 2 + r // 2) % 2) * 2 + (col + r) % 2) * levels + lev[k]
            gain, slot = shares[b], slots[b]
            wanted = []
            for e in range(2):
                g = jnp.where(core == 0, gain[e : e + 1], gain[1 - e : 2 - e])
                s = jnp.where(core == 0, slot[e : e + 1], slot[1 - e : 2 - e])
                wanted.append(jnp.where(s == place, g, 0.0))
            weights = jnp.concatenate(wanted, axis=0)
            chosen = jnp.where(weights > 0.0, 1.0, 0.0).astype(BF16)
            backs[r] = weights.T.astype(BF16)
            picked = jnp.dot(chosen, every[k, r], preferred_element_type=F32).astype(BF16)
            at = pl.ds(pl.multiple_of(r * cap, cap), cap)
            for e in range(2):
                xs[e, at] = picked[e * cap : (e + 1) * cap]
            return carry

        lax.fori_loop(0, columns, pick, 0)

        def expert(e, carry):
            @pl.when(e == 1)
            def _():
                middle()

            x = xs[e]
            gate = jnp.dot(x, wgs[e], preferred_element_type=F32)
            upper = jnp.dot(x, wus[e], preferred_element_type=F32)
            hidden = (gate / (1.0 + jnp.exp(-gate)) * upper).astype(BF16)
            ys[e] = jnp.dot(hidden, wds[e], preferred_element_type=F32).astype(BF16)
            return carry

        lax.fori_loop(0, 2, expert, 0)

        def mix(r, carry):
            at = pl.ds(pl.multiple_of(r * cap, cap), cap)
            y = jnp.concatenate([ys[e, at] for e in range(2)], axis=0)
            part[k, r] = jnp.dot(backs[r], y, preferred_element_type=F32).astype(BF16)
            return carry

        lax.fori_loop(0, columns, mix, 0)

    def fold_copies(g):
        k = g % levels
        p, q = part_rows if g < levels else tail_rows
        a, b = pl.ds(0, p.size), pl.ds(0, q.size)
        return [
            link(part.at[k, 3, p], first.at[g, 0, a], ps.at[g, 0], pr.at[g, 0], dev_x),
            link(part.at[k, 3, q], first.at[g, 1, b], ps.at[g, 1], pr.at[g, 1], dev_y),
            link(part.at[k, 1, p], first.at[g, 2, a], ps.at[g, 2], pr.at[g, 2], dev_x),
            link(part.at[k, 2, q], first.at[g, 3, b], ps.at[g, 3], pr.at[g, 3], dev_y),
            link(part.at[k, 2, p], second.at[g, 0, a], ps.at[g, 4], pr.at[g, 4], dev_y),
            link(part.at[k, 1, q], second.at[g, 1, b], ps.at[g, 5], pr.at[g, 5], dev_x),
        ]

    folds = [fold_copies(g) for g in range(levels + 1)]

    def fold_one(g):
        for i in range(4):
            folds[g][i].start()

    def fold_two(g):
        k = g % levels
        p, q = part_rows if g < levels else tail_rows
        for i, (r, piece) in enumerate(((2, p), (1, q))):
            folds[g][i].wait_recv()
            part[k, r, piece] = (
                part[k, r, piece].astype(F32) + first[g, i, pl.ds(0, piece.size)].astype(F32)
            ).astype(BF16)
            folds[g][4 + i].start()

    def fold_wait(g, i):
        folds[g][2 + i].wait_recv()
        folds[g][4 + i].wait_recv()

    def fold_sum(g, i):
        k = g % levels
        piece = (part_rows if g < levels else tail_rows)[i]
        at = pl.ds(0, piece.size)
        return (
            part[k, 0, piece].astype(F32) + first[g, 2 + i, at].astype(F32) + second[g, i, at].astype(F32)
        )

    def fold_three(g, i):
        fold_wait(g, i)
        if g == levels:
            out[tail_rows[i]] = fold_sum(g, i).astype(BF16)
        elif g:
            part[g, 0, part_rows[i]] = fold_sum(g, i).astype(BF16)

    def chain(view, land, s, r):
        send_end, send_mid = {}, {}
        for i in range(2):
            for k, end_slot, mid_slot in ((3, 0, 4), (2, 3, 1), (1, 2, 0)):
                send_end[k, i] = link(view(k, i), land(end_slot, i), s.at[k, i], r.at[end_slot, i], mate)
                send_mid[k, i] = link(
                    view(k, i), land(mid_slot, i), s.at[k, i], r.at[mid_slot, i], mate if k == 1 else inner
                )
        return send_end, send_mid, view, land, r

    def main_view(k, i):
        return part.at[k, 0, part_rows[i]]

    def tail_view(k, i):
        return part.at[k, pl.ds(0, columns), tail_rows[i]]

    rows_chain = chain(main_view, lambda slot, i: row_in.at[slot, part_rows[i]], cs, cr)
    tail_chain = chain(
        tail_view,
        lambda slot, i: plane_in.at[slot, pl.ds(0, columns), (pl.ds(0, bcut), pl.ds(bcut, spare - bcut))[i]],
        ds,
        dr,
    )

    def landed(c, slot, i):
        land, r = c[3], c[4]
        link(land(slot, i), land(slot, i), r.at[slot, i], r.at[slot, i], mate).wait_recv()

    def chain_mid(c, k, i):
        slot = {3: 3, 2: 2, 1: 4}[k]
        landed(c, slot, i)
        here = c[2](k, i)
        here[...] = (here[...].astype(F32) + c[3](slot, i)[...].astype(F32)).astype(BF16)
        c[1][k, i].start()

    def own_wait(c, i):
        landed(c, 0, i)

        @pl.when(mid == 1)
        def _():
            landed(c, 1, i)

    def own_rows(c, i):
        return c[3](0, i)[...].astype(F32) + jnp.where(mid == 1, c[3](1, i)[...].astype(F32), 0.0)

    def own_tail(i):
        own_wait(tail_chain, i)
        here = tail_view(0, i)
        here[...] = (here[...].astype(F32) + own_rows(tail_chain, i)).astype(BF16)

    def first_send():
        spread[0][0].start()
        spread[0][1].start()
        line_send(lines)
        on_mid(lambda: line_send_inner(lines))
        spread[0][2].start()
        spread[0][3].start()
        for copy in swap:
            copy.start()
        make_mine()
        hear_all()
        for copy in small:
            copy.start()

    def make_tables():
        for copy in small:
            copy.wait_recv()
        make_slots()
        for copy in keep:
            copy.wait()

    def swapped():
        for copy in swap:
            copy.wait_recv()

    def run(events):
        n = 0
        while n < len(events):
            who, stop = events[n][0], n + 1
            while stop < len(events) and events[stop][0] == who:
                stop += 1
            group = events[n:stop]

            def do(group=group):
                for event in group:
                    acts[event[1]](*event[2:])

            {"all": lambda f: f(), "end": on_end, "mid": on_mid}[who](do)
            n = stop

    acts = {
        "Start": first_send,
        "T": make_tables,
        "Swap": swapped,
        "Ss": spread_send,
        "Sr": spread_relay,
        "Sd": spread_done,
        "Lr": lambda k, i: line_relay(lines, k, i),
        "Lw": lambda k: line_wait(lines, k),
        "Bs": lambda: line_send(bands),
        "Bi": lambda: line_send_inner(bands),
        "Br": lambda k, i: line_relay(bands, k, i),
        "Bw": lambda k: line_wait(bands, k),
        "C": lambda k, hook: compute(k, lambda: run(hook)),
        "F1": fold_one,
        "F2": fold_two,
        "F3": fold_three,
        "De": lambda k, i: tail_chain[0][k, i].start(),
        "Dm": lambda k, i: chain_mid(tail_chain, k, i),
        "Dw": own_tail,
        "Ce": lambda k, i: rows_chain[0][k, i].start(),
        "Cm": lambda k, i: chain_mid(rows_chain, k, i),
        "Cw": lambda i: own_wait(rows_chain, i),
    }
    run(ORDER)
    for i, piece in enumerate(part_rows):
        out[piece] = (fold_sum(0, i) + own_rows(rows_chain, i)).astype(BF16)

    for group in spread + folds + [small, swap]:
        for copy in group:
            copy.wait_send()
    for i in range(2):
        for copies in (lines, bands):
            copies[i][0].wait_send()
        for c in (rows_chain, tail_chain):
            c[0][1, i].wait_send()
            c[0][2, i].wait_send()
            c[0][3, i].wait_send()

    @pl.when(mid == 1)
    def _():
        for i in range(2):
            for copies in (lines, bands):
                for copy in copies[i][1:5]:
                    copy.wait_send()


def on_layers(levels, tokens, expert_ids, route_weights, w_gate, w_up, w_down):
    tok_rows, width = tokens.shape
    top_count = expert_ids.shape[1]
    device_count = lax.axis_size("side") * levels
    capacity = 2 * tok_rows * top_count // device_count
    chips = device_count // 2
    columns = chips // levels
    spare = tok_rows // 4
    main = tok_rows - spare
    cut = (main // 2 + 7) // 8 * 8
    anywhere = pl.BlockSpec(memory_space=pl.ANY)
    vmem = pltpu.VMEM
    dma = pltpu.SemaphoreType.DMA
    return pl.pallas_call(
        functools.partial(fused_kernel, levels, spare),
        out_shape=jax.ShapeDtypeStruct((tok_rows, width), BF16),
        in_specs=[anywhere] * 6,
        out_specs=pl.BlockSpec(memory_space=vmem),
        scratch_shapes=[
            vmem((top_count, tok_rows), jnp.int32),
            vmem((top_count, tok_rows), F32),
            vmem((chips, 8, tok_rows), F32),
            vmem((chips, 8, tok_rows), F32),
            vmem((chips, 8, tok_rows), F32),
            vmem((2,) + w_gate.shape[1:], BF16),
            vmem((2,) + w_up.shape[1:], BF16),
            vmem((2,) + w_down.shape[1:], BF16),
            vmem((levels, columns, tok_rows, width), BF16),
            vmem((levels, columns, tok_rows, width), BF16),
            vmem((2, columns * capacity, width), BF16),
            vmem((2, columns * capacity, width), BF16),
            vmem((columns, tok_rows, 2 * capacity), BF16),
            vmem((levels + 1, 4, cut, width), BF16),
            vmem((levels + 1, 2, cut, width), BF16),
            vmem((5, main, width), BF16),
            vmem((5, columns, spare, width), BF16),
            dma((levels, 6)),
            dma((levels, 6)),
            dma((5, 2)),
            dma((4, 2)),
            dma((5, 2)),
            dma((4, 2)),
            dma((levels + 1, 6)),
            dma((levels + 1, 6)),
            dma((4, 2)),
            dma((5, 2)),
            dma((4, 2)),
            dma((5, 2)),
            dma((chips - 1,)),
            dma((chips - 1,)),
            dma((3,)),
            dma((3,)),
            pltpu.SemaphoreType.REGULAR((4,)),
            dma((6,)),
        ],
        compiler_params=pltpu.CompilerParams(
            collective_id=0, has_side_effects=True, vmem_limit_bytes=62 * 2**20
        ),
        name="layer",
    )(tokens, expert_ids.T, route_weights.T, w_gate, w_up, w_down)


def expert_ffn(rows, gate_proj, up_proj, down_proj):
    gate = jnp.dot(rows, gate_proj, preferred_element_type=jnp.float32)
    upper = jnp.dot(rows, up_proj, preferred_element_type=jnp.float32)
    hidden = (jax.nn.silu(gate) * upper).astype(jnp.bfloat16)
    return jnp.dot(hidden, down_proj, preferred_element_type=jnp.float32).astype(jnp.bfloat16)


def on_device(tokens, expert_ids, route_weights, w_gate, w_up, w_down):
    tok_rows = tokens.shape[0]
    width = tokens.shape[1]
    top_count = expert_ids.shape[1]
    side_count = lax.axis_size("side")
    device_count = side_count * lax.axis_size("lane")
    local_count = w_gate.shape[0]
    expert_count = device_count * local_count
    capacity = 2 * tok_rows * top_count // expert_count
    flat_ids = expert_ids.reshape(-1)
    onehot = (flat_ids[:, None] == jnp.arange(expert_count, dtype=jnp.int32)[None, :]).astype(
        jnp.int32
    )
    earlier = jnp.cumsum(onehot, axis=0) - onehot
    slot_index = jnp.sum(earlier * onehot, axis=1)
    position = (flat_ids * capacity + slot_index).reshape(tok_rows, top_count)
    buffer_rows = jnp.arange(expert_count * capacity, dtype=jnp.int32)
    dispatch_table = jnp.any(buffer_rows[:, None, None] == position[None, :, :], axis=2).astype(
        jnp.bfloat16
    )
    outgoing = jnp.dot(dispatch_table, tokens, preferred_element_type=jnp.float32).astype(
        jnp.bfloat16
    )
    outgoing = outgoing.reshape(expert_count, capacity, width)
    received = lax.all_to_all(outgoing, ("side", "lane"), split_axis=0, concat_axis=0, tiled=True)
    count = received.shape[1]
    grouped = received.reshape(device_count, local_count, count, width)
    rows = grouped[:, 0].reshape(device_count * count, width)
    output = expert_ffn(rows, w_gate[0], w_up[0], w_down[0])
    results = [output.reshape(device_count, count, width)]
    returned = lax.all_to_all(
        jnp.stack(results, axis=1).reshape(device_count * local_count, count, width),
        ("side", "lane"),
        split_axis=0,
        concat_axis=0,
        tiled=True,
    )
    flat_back = returned.reshape(expert_count * capacity, width)
    picked = flat_back[position]
    mixed = jnp.einsum("tk,tkd->td", route_weights, picked, preferred_element_type=jnp.float32)
    return mixed.astype(jnp.bfloat16)


def layered(mesh, tokens):
    side, levels = mesh.shape["side"], mesh.shape["lane"]
    layer_bytes = tokens.shape[0] // 2 * tokens.shape[1] * tokens.dtype.itemsize
    fits = 3 * layer_bytes < 32 * 2**20 and side * levels <= tokens.shape[0] // (side * levels) == 2**7
    return side == 2**3 and levels == 4 and fits


def solution(mesh):
    placed = (
        P(AXES, None),
        P(AXES, None),
        P(AXES, None),
        P(AXES, None, None),
        P(AXES, None, None),
        P(AXES, None, None),
    )

    def run(tokens, *rest):
        body = on_device
        if layered(mesh, tokens):
            body = functools.partial(on_layers, mesh.shape["lane"])
        return jax.shard_map(
            body, mesh=mesh, in_specs=placed, out_specs=P(AXES, None), check_vma=False
        )(tokens, *rest)

    return run
```

```python
import functools

import jax
import jax.numpy as jnp
from jax import lax
from jax.experimental import pallas as pl
from jax.experimental.pallas import tpu as pltpu
from jax.sharding import PartitionSpec as P

AXES = ("side", "lane")
MESH = pl.DeviceIdType.MESH
BF16 = jnp.bfloat16
F32 = jnp.float32


ORDER = [
    ("all", "Start"), ("end", "Sr", 0), ("end", "Lw", 3), ("end", "T"), ("end", "Ss", 3),
    ("end", "Lw", 1), ("end", "Ss", 1), ("end", "Sd", 0), ("end", "Bs"), ("mid", "Sr", 0),
    ("mid", "Lr", 1, 0), ("mid", "Lr", 2, 0), ("mid", "T"), ("mid", "Lr", 2, 1), ("mid", "Ss", 2),
    ("mid", "Lr", 1, 1), ("mid", "Sd", 0), ("mid", "Bi"), ("mid", "Ss", 1), ("mid", "Lr", 3, 0),
    ("all", "C", 0, [
        ("end", "Sr", 1), ("all", "Swap"),
    ]),
    ("end", "Lw", 2), ("end", "Ss", 2), ("end", "Sr", 2), ("end", "Bw", 1), ("end", "Sd", 1),
    ("end", "Sr", 3), ("mid", "Lr", 3, 1), ("mid", "Sr", 1), ("mid", "Sr", 2), ("mid", "Br", 2, 0),
    ("mid", "Br", 1, 0), ("mid", "Br", 2, 1), ("mid", "Ss", 3), ("mid", "Sd", 1), ("mid", "Br", 3, 0),
    ("mid", "Br", 1, 1),
    ("all", "C", 1, [
    ]),
    ("end", "De", 1, 1), ("end", "Bw", 2), ("end", "Sd", 2), ("end", "De", 1, 0), ("end", "F1", 1),
    ("mid", "Sd", 2), ("mid", "Br", 3, 1), ("mid", "Sr", 3), ("mid", "F1", 1),
    ("all", "C", 2, [
        ("end", "Sd", 3),
    ]),
    ("end", "F1", 2), ("end", "De", 2, 0), ("end", "De", 2, 1), ("end", "F2", 1), ("end", "Bw", 3),
    ("mid", "Bs"), ("mid", "Sd", 3),
    ("all", "C", 3, [
        ("mid", "Dm", 2, 1), ("mid", "F1", 2), ("mid", "Dm", 2, 0), ("mid", "F2", 1),
    ]),
    ("end", "De", 3, 0), ("end", "F2", 2), ("end", "F1", 3), ("end", "De", 3, 1), ("end", "F3", 2, 0),
    ("end", "Ce", 2, 0), ("end", "F3", 2, 1), ("end", "Ce", 2, 1), ("end", "F2", 3), ("end", "F1", 0),
    ("end", "F3", 1, 0), ("end", "Ce", 1, 0), ("end", "F3", 1, 1), ("end", "F3", 3, 1),
    ("end", "Dw", 0), ("end", "Ce", 1, 1), ("end", "F3", 3, 0), ("end", "Ce", 3, 1), ("end", "Dw", 1),
    ("end", "F1", 4), ("end", "F2", 0), ("end", "Ce", 3, 0), ("end", "F2", 4), ("end", "Cw", 1),
    ("end", "F3", 4, 1), ("end", "Cw", 0), ("end", "F3", 4, 0), ("end", "F3", 0, 0),
    ("end", "F3", 0, 1), ("mid", "F1", 3), ("mid", "Dm", 3, 0), ("mid", "Dm", 3, 1),
    ("mid", "Dm", 1, 0), ("mid", "F3", 1, 1), ("mid", "F2", 3), ("mid", "F2", 2), ("mid", "F3", 3, 0),
    ("mid", "Cm", 3, 0), ("mid", "F3", 3, 1), ("mid", "Dw", 1), ("mid", "Dm", 1, 1), ("mid", "Dw", 0),
    ("mid", "F1", 0), ("mid", "Cm", 3, 1), ("mid", "F3", 2, 1), ("mid", "F3", 1, 0), ("mid", "F1", 4),
    ("mid", "F3", 2, 0), ("mid", "Cm", 1, 0), ("mid", "F2", 0), ("mid", "Cm", 2, 0),
    ("mid", "Cm", 2, 1), ("mid", "Cm", 1, 1), ("mid", "F2", 4), ("mid", "Cw", 1), ("mid", "F3", 0, 0),
    ("mid", "F3", 0, 1), ("mid", "F3", 4, 1), ("mid", "F3", 4, 0), ("mid", "Cw", 0),
]


def flip(value, mask):
    bit = 1
    out = value
    while bit <= mask:
        if mask & bit:
            out = out + bit - 2 * bit * ((value // bit) % 2)
        bit *= 2
    return out


def fused_kernel(
    levels, spare, tokens, ids, gains, wg, wu, wd, out, ids_v, gains_v, mine, shares, slots, wgs, wus, wds, every,
    part, xs, ys, backs, first, second, row_in, plane_in, gs, gr, zs, zr, bs, br, ps, pr, cs, cr, ds, dr, ss, sr, ws,
    wr, known, local
):
    side, level = lax.axis_index("side"), lax.axis_index("lane")
    col, core = side // 2, side % 2
    mid = ((level + 1) // 2) % 2
    rows = out.shape[0]
    width = out.shape[1]
    chips = shares.shape[0]
    columns = chips // levels
    cap = xs.shape[1] // columns
    main = rows - spare
    cut = (main // 2 + 7) // 8 * 8
    bcut = (spare // 2 + 7) // 8 * 8
    whole = (pl.ds(0, rows // 2), pl.ds(rows // 2, rows // 2))
    part_rows = (pl.ds(0, cut), pl.ds(cut, main - cut))
    tail_rows = (pl.ds(main, bcut), pl.ds(main + bcut, spare - bcut))
    dev_x, dev_y = (flip(col, 1) * 2 + core, level), (flip(col, 2) * 2 + core, level)
    twin = (col * 2 + 1 - core, level)
    mate = (side, flip(level, 1))
    inner = (side, mid * flip(level, 3) + (1 - mid) * flip(level, 1))
    lev = [
        level,
        mid * flip(level, 1) + (1 - mid) * flip(level, 2),
        flip(level, 3),
        mid * flip(level, 2) + (1 - mid) * flip(level, 1),
    ]
    me = col * levels + level
    others = [(flip(col, m // levels), flip(level, m % levels)) for m in range(1, chips)]

    def on_mid(do):
        pl.when(mid == 1)(do)

    def on_end(do):
        pl.when(mid == 0)(do)

    def tell(sem, device):
        pl.semaphore_signal(sem, inc=1, device_id=device, device_id_type=MESH)

    barrier = pltpu.get_barrier_semaphore()
    for device in (dev_x, dev_y, mate, twin):
        tell(barrier, device)
    on_mid(lambda: tell(barrier, inner))
    fetch = [pltpu.make_async_copy(ids, ids_v, local.at[0]), pltpu.make_async_copy(gains, gains_v, local.at[1])]
    keep = [
        pltpu.make_async_copy(tokens, every.at[0, 0], local.at[2]),
        pltpu.make_async_copy(wg.at[0], wgs.at[0], local.at[3]),
        pltpu.make_async_copy(wu.at[0], wus.at[0], local.at[4]),
        pltpu.make_async_copy(wd.at[0], wds.at[0], local.at[5]),
    ]
    for copy in fetch + keep:
        copy.start()
    pl.semaphore_wait(barrier, 4 + mid)

    def make_mine():
        for copy in fetch:
            copy.wait()
        number = lax.broadcasted_iota(jnp.int32, (2 * chips, rows), 0)
        table = jnp.zeros((2 * chips, rows), F32)
        for k in range(ids_v.shape[0]):
            table = table + jnp.where(ids_v[k : k + 1] == number, gains_v[k : k + 1], 0.0)
        for q in range(columns):
            for z in range(levels):
                for c in range(2):
                    e = (q * 2 + c) * levels + z
                    mine[q * levels + z, c : c + 1, :] = table[e : e + 1, :]
                mine[q * levels + z, 2:8, :] = jnp.zeros((6, rows), F32)
        shares[me] = mine[me]

    def hear_all():
        for device in (dev_x, dev_y):
            tell(known.at[0], device)
        pl.semaphore_wait(known.at[0], 2)
        tell(known.at[1], mate)
        on_mid(lambda: tell(known.at[1], inner))
        pl.semaphore_wait(known.at[1], 1 + mid)

        @pl.when(mid == 1)
        def _():
            tell(known.at[2], mate)
            tell(known.at[2], inner)

        pl.semaphore_wait(known.at[2], 1)
        on_mid(lambda: tell(known.at[3], mate))
        on_end(lambda: pl.semaphore_wait(known.at[3], 1))

    def link(src, dst, s, r, device):
        return pltpu.make_async_remote_copy(
            src_ref=src, dst_ref=dst, send_sem=s, recv_sem=r, device_id=device, device_id_type=MESH
        )

    def spread_copies(k):
        p, q = whole if k == 0 else part_rows
        block = tokens if k == 0 else every.at[k, 0]
        return [
            link(block.at[p], every.at[k, 1, p], gs.at[k, 0], gr.at[k, 0], dev_x),
            link(block.at[q], every.at[k, 2, q], gs.at[k, 1], gr.at[k, 1], dev_y),
            link(block.at[q], every.at[k, 1, q], gs.at[k, 2], gr.at[k, 2], dev_x),
            link(block.at[p], every.at[k, 2, p], gs.at[k, 3], gr.at[k, 3], dev_y),
            link(every.at[k, 1, p], every.at[k, 3, p], gs.at[k, 4], gr.at[k, 4], dev_y),
            link(every.at[k, 2, q], every.at[k, 3, q], gs.at[k, 5], gr.at[k, 5], dev_x),
        ]

    spread = [spread_copies(k) for k in range(levels)]

    def spread_send(k):
        for i in range(4):
            spread[k][i].start()

    def spread_relay(k):
        spread[k][0].wait_recv()
        spread[k][4].start()
        spread[k][1].wait_recv()
        spread[k][5].start()

    def spread_done(k):
        for i in range(2, 6):
            spread[k][i].wait_recv()

    there = 1 + 2 * mid
    def line_copies(view, own, s, r):
        out = []
        for i in range(2):
            out.append(
                [
                    link(own(i), view(there, i), s.at[0, i], r.at[there, i], mate),
                    link(own(i), view(2, i), s.at[1, i], r.at[2, i], inner),
                    link(view(1, i), view(3, i), s.at[2, i], r.at[3, i], inner),
                    link(view(2, i), view(1, i), s.at[3, i], r.at[1, i], mate),
                    link(view(3, i), view(2, i), s.at[4, i], r.at[2, i], mate),
                    link(view(1, i), view(1, i), s.at[0, i], r.at[1, i], mate),
                    link(view(2, i), view(2, i), s.at[0, i], r.at[2, i], mate),
                    link(view(3, i), view(3, i), s.at[0, i], r.at[3, i], mate),
                ]
            )
        return out

    block_rows = (pl.ds(0, cut), pl.ds(cut, rows - cut))
    lines = line_copies(
        lambda k, i: every.at[k, 0, block_rows[i]], lambda i: tokens.at[block_rows[i]], zs, zr
    )

    def tails(k, i):
        return every.at[k, pl.ds(1, columns - 1), tail_rows[i]]

    bands = line_copies(tails, lambda i: tails(0, i), bs, br)

    def line_send(copies):
        for i in range(2):
            copies[i][0].start()

    def line_send_inner(copies):
        for i in range(2):
            copies[i][1].start()

    def line_wait(copies, k):
        for i in range(2):
            copies[i][k + 4].wait_recv()

    def line_relay(copies, k, i):
        copies[i][k + 4].wait_recv()
        copies[i][k + 1].start()

    small = [
        link(mine.at[q * levels + z], shares.at[me], ss.at[i], sr.at[i], (q * 2 + core, z))
        for i, (q, z) in enumerate(others)
    ]
    swap = [
        link(wg.at[0], wgs.at[1], ws.at[0], wr.at[0], twin),
        link(wu.at[0], wus.at[1], ws.at[1], wr.at[1], twin),
        link(wd.at[0], wds.at[1], ws.at[2], wr.at[2], twin),
    ]

    def make_slots():
        chosen = (shares[...] > 0.0).astype(F32).astype(BF16).reshape(chips * 8, rows)
        before = lax.broadcasted_iota(jnp.int32, (rows, rows), 0) < lax.broadcasted_iota(
            jnp.int32, (rows, rows), 1
        )
        before = before.astype(F32).astype(BF16)
        slots[...] = jnp.dot(chosen, before, preferred_element_type=F32).reshape(chips, 8, rows)

    def compute(k, middle):
        place = lax.broadcasted_iota(jnp.int32, (cap, rows), 0).astype(F32)

        def pick(r, carry):
            b = (((col // 2 + r // 2) % 2) * 2 + (col + r) % 2) * levels + lev[k]
            gain, slot = shares[b], slots[b]
            wanted = []
            for e in range(2):
                g = jnp.where(core == 0, gain[e : e + 1], gain[1 - e : 2 - e])
                s = jnp.where(core == 0, slot[e : e + 1], slot[1 - e : 2 - e])
                wanted.append(jnp.where(s == place, g, 0.0))
            weights = jnp.concatenate(wanted, axis=0)
            chosen = jnp.where(weights > 0.0, 1.0, 0.0).astype(BF16)
            backs[r] = weights.T.astype(BF16)
            picked = jnp.dot(chosen, every[k, r], preferred_element_type=F32).astype(BF16)
            at = pl.ds(pl.multiple_of(r * cap, cap), cap)
            for e in range(2):
                xs[e, at] = picked[e * cap : (e + 1) * cap]
            return carry

        lax.fori_loop(0, columns, pick, 0)

        def expert(e, carry):
            @pl.when(e == 1)
            def _():
                middle()

            x = xs[e]
            gate = jnp.dot(x, wgs[e], preferred_element_type=F32)
            upper = jnp.dot(x, wus[e], preferred_element_type=F32)
            hidden = (gate / (1.0 + jnp.exp(-gate)) * upper).astype(BF16)
            ys[e] = jnp.dot(hidden, wds[e], preferred_element_type=F32).astype(BF16)
            return carry

        lax.fori_loop(0, 2, expert, 0)

        def mix(r, carry):
            at = pl.ds(pl.multiple_of(r * cap, cap), cap)
            y = jnp.concatenate([ys[e, at] for e in range(2)], axis=0)
            part[k, r] = jnp.dot(backs[r], y, preferred_element_type=F32).astype(BF16)
            return carry

        lax.fori_loop(0, columns, mix, 0)

    def fold_copies(g):
        k = g % levels
        p, q = part_rows if g < levels else tail_rows
        a, b = pl.ds(0, p.size), pl.ds(0, q.size)
        return [
            link(part.at[k, 3, p], first.at[g, 0, a], ps.at[g, 0], pr.at[g, 0], dev_x),
            link(part.at[k, 3, q], first.at[g, 1, b], ps.at[g, 1], pr.at[g, 1], dev_y),
            link(part.at[k, 1, p], first.at[g, 2, a], ps.at[g, 2], pr.at[g, 2], dev_x),
            link(part.at[k, 2, q], first.at[g, 3, b], ps.at[g, 3], pr.at[g, 3], dev_y),
            link(part.at[k, 2, p], second.at[g, 0, a], ps.at[g, 4], pr.at[g, 4], dev_y),
            link(part.at[k, 1, q], second.at[g, 1, b], ps.at[g, 5], pr.at[g, 5], dev_x),
        ]

    folds = [fold_copies(g) for g in range(levels + 1)]

    def fold_one(g):
        for i in range(4):
            folds[g][i].start()

    def fold_two(g):
        k = g % levels
        p, q = part_rows if g < levels else tail_rows
        for i, (r, piece) in enumerate(((2, p), (1, q))):
            folds[g][i].wait_recv()
            part[k, r, piece] = (
                part[k, r, piece].astype(F32) + first[g, i, pl.ds(0, piece.size)].astype(F32)
            ).astype(BF16)
            folds[g][4 + i].start()

    def fold_wait(g, i):
        folds[g][2 + i].wait_recv()
        folds[g][4 + i].wait_recv()

    def fold_sum(g, i):
        k = g % levels
        piece = (part_rows if g < levels else tail_rows)[i]
        at = pl.ds(0, piece.size)
        return (
            part[k, 0, piece].astype(F32) + first[g, 2 + i, at].astype(F32) + second[g, i, at].astype(F32)
        )

    def fold_three(g, i):
        fold_wait(g, i)
        if g == levels:
            out[tail_rows[i]] = fold_sum(g, i).astype(BF16)
        elif g:
            part[g, 0, part_rows[i]] = fold_sum(g, i).astype(BF16)

    def chain(view, land, s, r):
        send_end, send_mid = {}, {}
        for i in range(2):
            for k, end_slot, mid_slot in ((3, 0, 4), (2, 3, 1), (1, 2, 0)):
                send_end[k, i] = link(view(k, i), land(end_slot, i), s.at[k, i], r.at[end_slot, i], mate)
                send_mid[k, i] = link(
                    view(k, i), land(mid_slot, i), s.at[k, i], r.at[mid_slot, i], mate if k == 1 else inner
                )
        return send_end, send_mid, view, land, r

    def main_view(k, i):
        return part.at[k, 0, part_rows[i]]

    def tail_view(k, i):
        return part.at[k, pl.ds(0, columns), tail_rows[i]]

    rows_chain = chain(main_view, lambda slot, i: row_in.at[slot, part_rows[i]], cs, cr)
    tail_chain = chain(
        tail_view,
        lambda slot, i: plane_in.at[slot, pl.ds(0, columns), (pl.ds(0, bcut), pl.ds(bcut, spare - bcut))[i]],
        ds,
        dr,
    )

    def landed(c, slot, i):
        land, r = c[3], c[4]
        link(land(slot, i), land(slot, i), r.at[slot, i], r.at[slot, i], mate).wait_recv()

    def chain_mid(c, k, i):
        slot = {3: 3, 2: 2, 1: 4}[k]
        landed(c, slot, i)
        here = c[2](k, i)
        here[...] = (here[...].astype(F32) + c[3](slot, i)[...].astype(F32)).astype(BF16)
        c[1][k, i].start()

    def own_wait(c, i):
        landed(c, 0, i)

        @pl.when(mid == 1)
        def _():
            landed(c, 1, i)

    def own_rows(c, i):
        return c[3](0, i)[...].astype(F32) + jnp.where(mid == 1, c[3](1, i)[...].astype(F32), 0.0)

    def own_tail(i):
        own_wait(tail_chain, i)
        here = tail_view(0, i)
        here[...] = (here[...].astype(F32) + own_rows(tail_chain, i)).astype(BF16)

    def first_send():
        spread[0][0].start()
        spread[0][1].start()
        line_send(lines)
        on_mid(lambda: line_send_inner(lines))
        spread[0][2].start()
        spread[0][3].start()
        for copy in swap:
            copy.start()
        make_mine()
        hear_all()
        for copy in small:
            copy.start()

    def make_tables():
        for copy in small:
            copy.wait_recv()
        make_slots()
        for copy in keep:
            copy.wait()

    def swapped():
        for copy in swap:
            copy.wait_recv()

    def run(events):
        n = 0
        while n < len(events):
            who, stop = events[n][0], n + 1
            while stop < len(events) and events[stop][0] == who:
                stop += 1
            group = events[n:stop]

            def do(group=group):
                for event in group:
                    acts[event[1]](*event[2:])

            {"all": lambda f: f(), "end": on_end, "mid": on_mid}[who](do)
            n = stop

    acts = {
        "Start": first_send,
        "T": make_tables,
        "Swap": swapped,
        "Ss": spread_send,
        "Sr": spread_relay,
        "Sd": spread_done,
        "Lr": lambda k, i: line_relay(lines, k, i),
        "Lw": lambda k: line_wait(lines, k),
        "Bs": lambda: line_send(bands),
        "Bi": lambda: line_send_inner(bands),
        "Br": lambda k, i: line_relay(bands, k, i),
        "Bw": lambda k: line_wait(bands, k),
        "C": lambda k, hook: compute(k, lambda: run(hook)),
        "F1": fold_one,
        "F2": fold_two,
        "F3": fold_three,
        "De": lambda k, i: tail_chain[0][k, i].start(),
        "Dm": lambda k, i: chain_mid(tail_chain, k, i),
        "Dw": own_tail,
        "Ce": lambda k, i: rows_chain[0][k, i].start(),
        "Cm": lambda k, i: chain_mid(rows_chain, k, i),
        "Cw": lambda i: own_wait(rows_chain, i),
    }
    run(ORDER)
    for i, piece in enumerate(part_rows):
        out[piece] = (fold_sum(0, i) + own_rows(rows_chain, i)).astype(BF16)

    for group in spread + folds + [small, swap]:
        for copy in group:
            copy.wait_send()
    for i in range(2):
        for copies in (lines, bands):
            copies[i][0].wait_send()
        for c in (rows_chain, tail_chain):
            c[0][1, i].wait_send()
            c[0][2, i].wait_send()
            c[0][3, i].wait_send()

    @pl.when(mid == 1)
    def _():
        for i in range(2):
            for copies in (lines, bands):
                for copy in copies[i][1:5]:
                    copy.wait_send()


def on_layers(levels, tokens, expert_ids, route_weights, w_gate, w_up, w_down):
    tok_rows, width = tokens.shape
    top_count = expert_ids.shape[1]
    device_count = lax.axis_size("side") * levels
    capacity = 2 * tok_rows * top_count // device_count
    chips = device_count // 2
    columns = chips // levels
    spare = tok_rows // 4
    main = tok_rows - spare
    cut = (main // 2 + 7) // 8 * 8
    anywhere = pl.BlockSpec(memory_space=pl.ANY)
    vmem = pltpu.VMEM
    dma = pltpu.SemaphoreType.DMA
    return pl.pallas_call(
        functools.partial(fused_kernel, levels, spare),
        out_shape=jax.ShapeDtypeStruct((tok_rows, width), BF16),
        in_specs=[anywhere] * 6,
        out_specs=pl.BlockSpec(memory_space=vmem),
        scratch_shapes=[
            vmem((top_count, tok_rows), jnp.int32),
            vmem((top_count, tok_rows), F32),
            vmem((chips, 8, tok_rows), F32),
            vmem((chips, 8, tok_rows), F32),
            vmem((chips, 8, tok_rows), F32),
            vmem((2,) + w_gate.shape[1:], BF16),
            vmem((2,) + w_up.shape[1:], BF16),
            vmem((2,) + w_down.shape[1:], BF16),
            vmem((levels, columns, tok_rows, width), BF16),
            vmem((levels, columns, tok_rows, width), BF16),
            vmem((2, columns * capacity, width), BF16),
            vmem((2, columns * capacity, width), BF16),
            vmem((columns, tok_rows, 2 * capacity), BF16),
            vmem((levels + 1, 4, cut, width), BF16),
            vmem((levels + 1, 2, cut, width), BF16),
            vmem((5, main, width), BF16),
            vmem((5, columns, spare, width), BF16),
            dma((levels, 6)),
            dma((levels, 6)),
            dma((5, 2)),
            dma((4, 2)),
            dma((5, 2)),
            dma((4, 2)),
            dma((levels + 1, 6)),
            dma((levels + 1, 6)),
            dma((4, 2)),
            dma((5, 2)),
            dma((4, 2)),
            dma((5, 2)),
            dma((chips - 1,)),
            dma((chips - 1,)),
            dma((3,)),
            dma((3,)),
            pltpu.SemaphoreType.REGULAR((4,)),
            dma((6,)),
        ],
        compiler_params=pltpu.CompilerParams(
            collective_id=0, has_side_effects=True, vmem_limit_bytes=53 * 2**20
        ),
        name="layer",
    )(tokens, expert_ids.T, route_weights.T, w_gate, w_up, w_down)


def expert_ffn(rows, gate_proj, up_proj, down_proj):
    gate = jnp.dot(rows, gate_proj, preferred_element_type=jnp.float32)
    upper = jnp.dot(rows, up_proj, preferred_element_type=jnp.float32)
    hidden = (jax.nn.silu(gate) * upper).astype(jnp.bfloat16)
    return jnp.dot(hidden, down_proj, preferred_element_type=jnp.float32).astype(jnp.bfloat16)


def on_device(tokens, expert_ids, route_weights, w_gate, w_up, w_down):
    tok_rows = tokens.shape[0]
    width = tokens.shape[1]
    top_count = expert_ids.shape[1]
    side_count = lax.axis_size("side")
    device_count = side_count * lax.axis_size("lane")
    local_count = w_gate.shape[0]
    expert_count = device_count * local_count
    capacity = 2 * tok_rows * top_count // expert_count
    flat_ids = expert_ids.reshape(-1)
    onehot = (flat_ids[:, None] == jnp.arange(expert_count, dtype=jnp.int32)[None, :]).astype(
        jnp.int32
    )
    earlier = jnp.cumsum(onehot, axis=0) - onehot
    slot_index = jnp.sum(earlier * onehot, axis=1)
    position = (flat_ids * capacity + slot_index).reshape(tok_rows, top_count)
    buffer_rows = jnp.arange(expert_count * capacity, dtype=jnp.int32)
    dispatch_table = jnp.any(buffer_rows[:, None, None] == position[None, :, :], axis=2).astype(
        jnp.bfloat16
    )
    outgoing = jnp.dot(dispatch_table, tokens, preferred_element_type=jnp.float32).astype(
        jnp.bfloat16
    )
    outgoing = outgoing.reshape(expert_count, capacity, width)
    received = lax.all_to_all(outgoing, ("side", "lane"), split_axis=0, concat_axis=0, tiled=True)
    count = received.shape[1]
    grouped = received.reshape(device_count, local_count, count, width)
    rows = grouped[:, 0].reshape(device_count * count, width)
    output = expert_ffn(rows, w_gate[0], w_up[0], w_down[0])
    results = [output.reshape(device_count, count, width)]
    returned = lax.all_to_all(
        jnp.stack(results, axis=1).reshape(device_count * local_count, count, width),
        ("side", "lane"),
        split_axis=0,
        concat_axis=0,
        tiled=True,
    )
    flat_back = returned.reshape(expert_count * capacity, width)
    picked = flat_back[position]
    mixed = jnp.einsum("tk,tkd->td", route_weights, picked, preferred_element_type=jnp.float32)
    return mixed.astype(jnp.bfloat16)


def layered(mesh, tokens):
    side, levels = mesh.shape["side"], mesh.shape["lane"]
    layer_bytes = tokens.shape[0] // 2 * tokens.shape[1] * tokens.dtype.itemsize
    fits = 3 * layer_bytes < 32 * 2**20 and side * levels <= tokens.shape[0] // (side * levels) == 2**7
    return side == 2**3 and levels == 4 and fits


def solution(mesh):
    placed = (
        P(AXES, None),
        P(AXES, None),
        P(AXES, None),
        P(AXES, None, None),
        P(AXES, None, None),
        P(AXES, None, None),
    )

    def run(tokens, *rest):
        body = on_device
        if layered(mesh, tokens):
            body = functools.partial(on_layers, mesh.shape["lane"])
        return jax.shard_map(
            body, mesh=mesh, in_specs=placed, out_specs=P(AXES, None), check_vma=False
        )(tokens, *rest)

    return run
```

```python
import functools

import jax
import jax.numpy as jnp
from jax import lax
from jax.experimental import pallas as pl
from jax.experimental.pallas import tpu as pltpu
from jax.sharding import PartitionSpec as P

AXES = ("side", "lane")
MESH = pl.DeviceIdType.MESH
BF16 = jnp.bfloat16
F32 = jnp.float32


ORDER = [
    ("all", "Start"), ("end", "Sr", 0), ("end", "Lw", 3), ("end", "T"), ("end", "Ss", 3),
    ("end", "Lw", 1), ("end", "Ss", 1), ("end", "Sd", 0), ("end", "Bs"), ("mid", "Sr", 0),
    ("mid", "Lr", 1, 0), ("mid", "Lr", 2, 0), ("mid", "T"), ("mid", "Lr", 2, 1), ("mid", "Ss", 2),
    ("mid", "Lr", 1, 1), ("mid", "Sd", 0), ("mid", "Bi"), ("mid", "Ss", 1), ("mid", "Lr", 3, 0),
    ("all", "C", 0, [
        ("end", "Sr", 1), ("all", "Swap"),
    ]),
    ("end", "Lw", 2), ("end", "Ss", 2), ("end", "Sr", 2), ("end", "Bw", 1), ("end", "Sd", 1),
    ("end", "Sr", 3), ("mid", "Lr", 3, 1), ("mid", "Sr", 1), ("mid", "Sr", 2), ("mid", "Br", 2, 0),
    ("mid", "Br", 1, 0), ("mid", "Br", 2, 1), ("mid", "Ss", 3), ("mid", "Sd", 1), ("mid", "Br", 3, 0),
    ("mid", "Br", 1, 1),
    ("all", "C", 1, [
    ]),
    ("end", "De", 1, 1), ("end", "Bw", 2), ("end", "Sd", 2), ("end", "De", 1, 0), ("end", "F1", 1),
    ("mid", "Sd", 2), ("mid", "Br", 3, 1), ("mid", "Sr", 3), ("mid", "F1", 1),
    ("all", "C", 2, [
        ("end", "Sd", 3),
    ]),
    ("end", "F1", 2), ("end", "De", 2, 0), ("end", "De", 2, 1), ("end", "F2", 1), ("end", "Bw", 3),
    ("mid", "Bs"), ("mid", "Sd", 3),
    ("all", "C", 3, [
        ("mid", "Dm", 2, 1), ("mid", "F1", 2), ("mid", "Dm", 2, 0), ("mid", "F2", 1),
    ]),
    ("end", "De", 3, 0), ("end", "F2", 2), ("end", "F1", 3), ("end", "De", 3, 1), ("end", "F3", 2, 0),
    ("end", "Ce", 2, 0), ("end", "F3", 2, 1), ("end", "Ce", 2, 1), ("end", "F2", 3), ("end", "F1", 0),
    ("end", "F3", 1, 0), ("end", "Ce", 1, 0), ("end", "F3", 1, 1), ("end", "F3", 3, 1),
    ("end", "Dw", 0), ("end", "Ce", 1, 1), ("end", "F3", 3, 0), ("end", "Ce", 3, 1), ("end", "Dw", 1),
    ("end", "F1", 4), ("end", "F2", 0), ("end", "Ce", 3, 0), ("end", "F2", 4), ("end", "Cw", 1),
    ("end", "F3", 4, 1), ("end", "Cw", 0), ("end", "F3", 4, 0), ("end", "F3", 0, 0),
    ("end", "F3", 0, 1), ("mid", "F1", 3), ("mid", "Dm", 3, 0), ("mid", "Dm", 3, 1),
    ("mid", "Dm", 1, 0), ("mid", "F3", 1, 1), ("mid", "F2", 3), ("mid", "F2", 2), ("mid", "F3", 3, 0),
    ("mid", "Cm", 3, 0), ("mid", "F3", 3, 1), ("mid", "Dw", 1), ("mid", "Dm", 1, 1), ("mid", "Dw", 0),
    ("mid", "F1", 0), ("mid", "Cm", 3, 1), ("mid", "F3", 2, 1), ("mid", "F3", 1, 0), ("mid", "F1", 4),
    ("mid", "F3", 2, 0), ("mid", "Cm", 1, 0), ("mid", "F2", 0), ("mid", "Cm", 2, 0),
    ("mid", "Cm", 2, 1), ("mid", "Cm", 1, 1), ("mid", "F2", 4), ("mid", "Cw", 1), ("mid", "F3", 0, 0),
    ("mid", "F3", 0, 1), ("mid", "F3", 4, 1), ("mid", "F3", 4, 0), ("mid", "Cw", 0),
]


def flip(value, mask):
    bit = 1
    out = value
    while bit <= mask:
        if mask & bit:
            out = out + bit - 2 * bit * ((value // bit) % 2)
        bit *= 2
    return out


def fused_kernel(
    levels, spare, tokens, ids, gains, wg, wu, wd, out, ids_v, gains_v, mine, shares, slots, wgs, wus, wds, every,
    part, xs, ys, backs, first, second, row_in, plane_in, gs, gr, zs, zr, bs, br, ps, pr, cs, cr, ds, dr, ss, sr, ws,
    wr, known, local
):
    side, level = lax.axis_index("side"), lax.axis_index("lane")
    col, core = side // 2, side % 2
    mid = ((level + 1) // 2) % 2
    rows = out.shape[0]
    width = out.shape[1]
    chips = shares.shape[0]
    columns = chips // levels
    cap = xs.shape[1] // columns
    main = rows - spare
    cut = (main // 2 + 7) // 8 * 8
    bcut = (spare // 2 + 7) // 8 * 8
    whole = (pl.ds(0, rows // 2), pl.ds(rows // 2, rows // 2))
    part_rows = (pl.ds(0, cut), pl.ds(cut, main - cut))
    tail_rows = (pl.ds(main, bcut), pl.ds(main + bcut, spare - bcut))
    dev_x, dev_y = (flip(col, 1) * 2 + core, level), (flip(col, 2) * 2 + core, level)
    twin = (col * 2 + 1 - core, level)
    mate = (side, flip(level, 1))
    inner = (side, mid * flip(level, 3) + (1 - mid) * flip(level, 1))
    lev = [
        level,
        mid * flip(level, 1) + (1 - mid) * flip(level, 2),
        flip(level, 3),
        mid * flip(level, 2) + (1 - mid) * flip(level, 1),
    ]
    me = col * levels + level
    others = [(flip(col, m // levels), flip(level, m % levels)) for m in range(1, chips)]

    def on_mid(do):
        pl.when(mid == 1)(do)

    def on_end(do):
        pl.when(mid == 0)(do)

    def tell(sem, device):
        pl.semaphore_signal(sem, inc=1, device_id=device, device_id_type=MESH)

    barrier = pltpu.get_barrier_semaphore()
    for device in (dev_x, dev_y, mate, twin):
        tell(barrier, device)
    on_mid(lambda: tell(barrier, inner))
    fetch = [pltpu.make_async_copy(ids, ids_v, local.at[0]), pltpu.make_async_copy(gains, gains_v, local.at[1])]
    keep = [
        pltpu.make_async_copy(tokens, every.at[0, 0], local.at[2]),
        pltpu.make_async_copy(wg.at[0], wgs.at[0], local.at[3]),
        pltpu.make_async_copy(wu.at[0], wus.at[0], local.at[4]),
        pltpu.make_async_copy(wd.at[0], wds.at[0], local.at[5]),
    ]
    for copy in fetch + keep:
        copy.start()
    pl.semaphore_wait(barrier, 4 + mid)

    def make_mine():
        for copy in fetch:
            copy.wait()
        number = lax.broadcasted_iota(jnp.int32, (2 * chips, rows), 0)
        table = jnp.zeros((2 * chips, rows), F32)
        for k in range(ids_v.shape[0]):
            table = table + jnp.where(ids_v[k : k + 1] == number, gains_v[k : k + 1], 0.0)
        for q in range(columns):
            for z in range(levels):
                for c in range(2):
                    e = (q * 2 + c) * levels + z
                    mine[q * levels + z, c : c + 1, :] = table[e : e + 1, :]
                mine[q * levels + z, 2:8, :] = jnp.zeros((6, rows), F32)
        shares[me] = mine[me]

    def hear_all():
        for device in (dev_x, dev_y):
            tell(known.at[0], device)
        pl.semaphore_wait(known.at[0], 2)
        tell(known.at[1], mate)
        on_mid(lambda: tell(known.at[1], inner))
        pl.semaphore_wait(known.at[1], 1 + mid)

        @pl.when(mid == 1)
        def _():
            tell(known.at[2], mate)
            tell(known.at[2], inner)

        pl.semaphore_wait(known.at[2], 1)
        on_mid(lambda: tell(known.at[3], mate))
        on_end(lambda: pl.semaphore_wait(known.at[3], 1))

    def link(src, dst, s, r, device):
        return pltpu.make_async_remote_copy(
            src_ref=src, dst_ref=dst, send_sem=s, recv_sem=r, device_id=device, device_id_type=MESH
        )

    def spread_copies(k):
        p, q = whole if k == 0 else part_rows
        block = tokens if k == 0 else every.at[k, 0]
        return [
            link(block.at[p], every.at[k, 1, p], gs.at[k, 0], gr.at[k, 0], dev_x),
            link(block.at[q], every.at[k, 2, q], gs.at[k, 1], gr.at[k, 1], dev_y),
            link(block.at[q], every.at[k, 1, q], gs.at[k, 2], gr.at[k, 2], dev_x),
            link(block.at[p], every.at[k, 2, p], gs.at[k, 3], gr.at[k, 3], dev_y),
            link(every.at[k, 1, p], every.at[k, 3, p], gs.at[k, 4], gr.at[k, 4], dev_y),
            link(every.at[k, 2, q], every.at[k, 3, q], gs.at[k, 5], gr.at[k, 5], dev_x),
        ]

    spread = [spread_copies(k) for k in range(levels)]

    def spread_send(k):
        for i in range(4):
            spread[k][i].start()

    def spread_relay(k):
        spread[k][0].wait_recv()
        spread[k][4].start()
        spread[k][1].wait_recv()
        spread[k][5].start()

    def spread_done(k):
        for i in range(2, 6):
            spread[k][i].wait_recv()

    there = 1 + 2 * mid
    def line_copies(view, own, s, r):
        out = []
        for i in range(2):
            out.append(
                [
                    link(own(i), view(there, i), s.at[0, i], r.at[there, i], mate),
                    link(own(i), view(2, i), s.at[1, i], r.at[2, i], inner),
                    link(view(1, i), view(3, i), s.at[2, i], r.at[3, i], inner),
                    link(view(2, i), view(1, i), s.at[3, i], r.at[1, i], mate),
                    link(view(3, i), view(2, i), s.at[4, i], r.at[2, i], mate),
                    link(view(1, i), view(1, i), s.at[0, i], r.at[1, i], mate),
                    link(view(2, i), view(2, i), s.at[0, i], r.at[2, i], mate),
                    link(view(3, i), view(3, i), s.at[0, i], r.at[3, i], mate),
                ]
            )
        return out

    block_rows = (pl.ds(0, cut), pl.ds(cut, rows - cut))
    lines = line_copies(
        lambda k, i: every.at[k, 0, block_rows[i]], lambda i: tokens.at[block_rows[i]], zs, zr
    )

    def tails(k, i):
        return every.at[k, pl.ds(1, columns - 1), tail_rows[i]]

    bands = line_copies(tails, lambda i: tails(0, i), bs, br)

    def line_send(copies):
        for i in range(2):
            copies[i][0].start()

    def line_send_inner(copies):
        for i in range(2):
            copies[i][1].start()

    def line_wait(copies, k):
        for i in range(2):
            copies[i][k + 4].wait_recv()

    def line_relay(copies, k, i):
        copies[i][k + 4].wait_recv()
        copies[i][k + 1].start()

    small = [
        link(mine.at[q * levels + z], shares.at[me], ss.at[i], sr.at[i], (q * 2 + core, z))
        for i, (q, z) in enumerate(others)
    ]
    swap = [
        link(wg.at[0], wgs.at[1], ws.at[0], wr.at[0], twin),
        link(wu.at[0], wus.at[1], ws.at[1], wr.at[1], twin),
        link(wd.at[0], wds.at[1], ws.at[2], wr.at[2], twin),
    ]

    def make_slots():
        chosen = (shares[...] > 0.0).astype(F32).astype(BF16).reshape(chips * 8, rows)
        before = lax.broadcasted_iota(jnp.int32, (rows, rows), 0) < lax.broadcasted_iota(
            jnp.int32, (rows, rows), 1
        )
        before = before.astype(F32).astype(BF16)
        slots[...] = jnp.dot(chosen, before, preferred_element_type=F32).reshape(chips, 8, rows)

    def compute(k, middle):
        place = lax.broadcasted_iota(jnp.int32, (cap, rows), 0).astype(F32)

        def pick(r, carry):
            b = (((col // 2 + r // 2) % 2) * 2 + (col + r) % 2) * levels + lev[k]
            gain, slot = shares[b], slots[b]
            wanted = []
            for e in range(2):
                g = jnp.where(core == 0, gain[e : e + 1], gain[1 - e : 2 - e])
                s = jnp.where(core == 0, slot[e : e + 1], slot[1 - e : 2 - e])
                wanted.append(jnp.where(s == place, g, 0.0))
            weights = jnp.concatenate(wanted, axis=0)
            chosen = jnp.where(weights > 0.0, 1.0, 0.0).astype(BF16)
            backs[r] = weights.T.astype(BF16)
            picked = jnp.dot(chosen, every[k, r], preferred_element_type=F32).astype(BF16)
            at = pl.ds(pl.multiple_of(r * cap, cap), cap)
            for e in range(2):
                xs[e, at] = picked[e * cap : (e + 1) * cap]
            return carry

        lax.fori_loop(0, columns, pick, 0)

        def expert(e, carry):
            @pl.when(e == 1)
            def _():
                middle()

            x = xs[e]
            gate = jnp.dot(x, wgs[e], preferred_element_type=F32)
            upper = jnp.dot(x, wus[e], preferred_element_type=F32)
            hidden = (gate / (1.0 + jnp.exp(-gate)) * upper).astype(BF16)
            ys[e] = jnp.dot(hidden, wds[e], preferred_element_type=F32).astype(BF16)
            return carry

        lax.fori_loop(0, 2, expert, 0)

        def mix(r, carry):
            at = pl.ds(pl.multiple_of(r * cap, cap), cap)
            y = jnp.concatenate([ys[e, at] for e in range(2)], axis=0)
            part[k, r] = jnp.dot(backs[r], y, preferred_element_type=F32).astype(BF16)
            return carry

        lax.fori_loop(0, columns, mix, 0)

    def fold_copies(g):
        k = g % levels
        p, q = part_rows if g < levels else tail_rows
        a, b = pl.ds(0, p.size), pl.ds(0, q.size)
        return [
            link(part.at[k, 3, p], first.at[g, 0, a], ps.at[g, 0], pr.at[g, 0], dev_x),
            link(part.at[k, 3, q], first.at[g, 1, b], ps.at[g, 1], pr.at[g, 1], dev_y),
            link(part.at[k, 1, p], first.at[g, 2, a], ps.at[g, 2], pr.at[g, 2], dev_x),
            link(part.at[k, 2, q], first.at[g, 3, b], ps.at[g, 3], pr.at[g, 3], dev_y),
            link(part.at[k, 2, p], second.at[g, 0, a], ps.at[g, 4], pr.at[g, 4], dev_y),
            link(part.at[k, 1, q], second.at[g, 1, b], ps.at[g, 5], pr.at[g, 5], dev_x),
        ]

    folds = [fold_copies(g) for g in range(levels + 1)]

    def fold_one(g):
        for i in range(4):
            folds[g][i].start()

    def fold_two(g):
        k = g % levels
        p, q = part_rows if g < levels else tail_rows
        for i, (r, piece) in enumerate(((2, p), (1, q))):
            folds[g][i].wait_recv()
            part[k, r, piece] = (
                part[k, r, piece].astype(F32) + first[g, i, pl.ds(0, piece.size)].astype(F32)
            ).astype(BF16)
            folds[g][4 + i].start()

    def fold_wait(g, i):
        folds[g][2 + i].wait_recv()
        folds[g][4 + i].wait_recv()

    def fold_sum(g, i):
        k = g % levels
        piece = (part_rows if g < levels else tail_rows)[i]
        at = pl.ds(0, piece.size)
        return (
            part[k, 0, piece].astype(F32) + first[g, 2 + i, at].astype(F32) + second[g, i, at].astype(F32)
        )

    def fold_three(g, i):
        fold_wait(g, i)
        if g == levels:
            out[tail_rows[i]] = fold_sum(g, i).astype(BF16)
        elif g:
            part[g, 0, part_rows[i]] = fold_sum(g, i).astype(BF16)

    def chain(view, land, s, r):
        send_end, send_mid = {}, {}
        for i in range(2):
            for k, end_slot, mid_slot in ((3, 0, 4), (2, 3, 1), (1, 2, 0)):
                send_end[k, i] = link(view(k, i), land(end_slot, i), s.at[k, i], r.at[end_slot, i], mate)
                send_mid[k, i] = link(
                    view(k, i), land(mid_slot, i), s.at[k, i], r.at[mid_slot, i], mate if k == 1 else inner
                )
        return send_end, send_mid, view, land, r

    def main_view(k, i):
        return part.at[k, 0, part_rows[i]]

    def tail_view(k, i):
        return part.at[k, pl.ds(0, columns), tail_rows[i]]

    rows_chain = chain(main_view, lambda slot, i: row_in.at[slot, part_rows[i]], cs, cr)
    tail_chain = chain(
        tail_view,
        lambda slot, i: plane_in.at[slot, pl.ds(0, columns), (pl.ds(0, bcut), pl.ds(bcut, spare - bcut))[i]],
        ds,
        dr,
    )

    def landed(c, slot, i):
        land, r = c[3], c[4]
        link(land(slot, i), land(slot, i), r.at[slot, i], r.at[slot, i], mate).wait_recv()

    def chain_mid(c, k, i):
        slot = {3: 3, 2: 2, 1: 4}[k]
        landed(c, slot, i)
        here = c[2](k, i)
        here[...] = (here[...].astype(F32) + c[3](slot, i)[...].astype(F32)).astype(BF16)
        c[1][k, i].start()

    def own_wait(c, i):
        landed(c, 0, i)

        @pl.when(mid == 1)
        def _():
            landed(c, 1, i)

    def own_rows(c, i):
        return c[3](0, i)[...].astype(F32) + jnp.where(mid == 1, c[3](1, i)[...].astype(F32), 0.0)

    def own_tail(i):
        own_wait(tail_chain, i)
        here = tail_view(0, i)
        here[...] = (here[...].astype(F32) + own_rows(tail_chain, i)).astype(BF16)

    def first_send():
        spread[0][0].start()
        spread[0][1].start()
        line_send(lines)
        on_mid(lambda: line_send_inner(lines))
        spread[0][2].start()
        spread[0][3].start()
        for copy in swap:
            copy.start()
        make_mine()
        hear_all()
        for copy in small:
            copy.start()

    def make_tables():
        for copy in small:
            copy.wait_recv()
        make_slots()
        for copy in keep:
            copy.wait()

    def swapped():
        for copy in swap:
            copy.wait_recv()

    def run(events):
        n = 0
        while n < len(events):
            who, stop = events[n][0], n + 1
            while stop < len(events) and events[stop][0] == who:
                stop += 1
            group = events[n:stop]

            def do(group=group):
                for event in group:
                    acts[event[1]](*event[2:])

            {"all": lambda f: f(), "end": on_end, "mid": on_mid}[who](do)
            n = stop

    acts = {
        "Start": first_send,
        "T": make_tables,
        "Swap": swapped,
        "Ss": spread_send,
        "Sr": spread_relay,
        "Sd": spread_done,
        "Lr": lambda k, i: line_relay(lines, k, i),
        "Lw": lambda k: line_wait(lines, k),
        "Bs": lambda: line_send(bands),
        "Bi": lambda: line_send_inner(bands),
        "Br": lambda k, i: line_relay(bands, k, i),
        "Bw": lambda k: line_wait(bands, k),
        "C": lambda k, hook: compute(k, lambda: run(hook)),
        "F1": fold_one,
        "F2": fold_two,
        "F3": fold_three,
        "De": lambda k, i: tail_chain[0][k, i].start(),
        "Dm": lambda k, i: chain_mid(tail_chain, k, i),
        "Dw": own_tail,
        "Ce": lambda k, i: rows_chain[0][k, i].start(),
        "Cm": lambda k, i: chain_mid(rows_chain, k, i),
        "Cw": lambda i: own_wait(rows_chain, i),
    }
    run(ORDER)
    for i, piece in enumerate(part_rows):
        out[piece] = (fold_sum(0, i) + own_rows(rows_chain, i)).astype(BF16)

    for group in spread + folds + [small, swap]:
        for copy in group:
            copy.wait_send()
    for i in range(2):
        for copies in (lines, bands):
            copies[i][0].wait_send()
        for c in (rows_chain, tail_chain):
            c[0][1, i].wait_send()
            c[0][2, i].wait_send()
            c[0][3, i].wait_send()

    @pl.when(mid == 1)
    def _():
        for i in range(2):
            for copies in (lines, bands):
                for copy in copies[i][1:5]:
                    copy.wait_send()


def on_layers(levels, tokens, expert_ids, route_weights, w_gate, w_up, w_down):
    tok_rows, width = tokens.shape
    top_count = expert_ids.shape[1]
    device_count = lax.axis_size("side") * levels
    capacity = 2 * tok_rows * top_count // device_count
    chips = device_count // 2
    columns = chips // levels
    spare = tok_rows // 4
    main = tok_rows - spare
    cut = (main // 2 + 7) // 8 * 8
    anywhere = pl.BlockSpec(memory_space=pl.ANY)
    stay = functools.partial(pltpu.with_memory_space_constraint, memory_space=pltpu.HBM)
    vmem = pltpu.VMEM
    dma = pltpu.SemaphoreType.DMA
    return pl.pallas_call(
        functools.partial(fused_kernel, levels, spare),
        out_shape=jax.ShapeDtypeStruct((tok_rows, width), BF16),
        in_specs=[anywhere] * 6,
        out_specs=pl.BlockSpec(memory_space=vmem),
        scratch_shapes=[
            vmem((top_count, tok_rows), jnp.int32),
            vmem((top_count, tok_rows), F32),
            vmem((chips, 8, tok_rows), F32),
            vmem((chips, 8, tok_rows), F32),
            vmem((chips, 8, tok_rows), F32),
            vmem((2,) + w_gate.shape[1:], BF16),
            vmem((2,) + w_up.shape[1:], BF16),
            vmem((2,) + w_down.shape[1:], BF16),
            vmem((levels, columns, tok_rows, width), BF16),
            vmem((levels, columns, tok_rows, width), BF16),
            vmem((2, columns * capacity, width), BF16),
            vmem((2, columns * capacity, width), BF16),
            vmem((columns, tok_rows, 2 * capacity), BF16),
            vmem((levels + 1, 4, cut, width), BF16),
            vmem((levels + 1, 2, cut, width), BF16),
            vmem((5, main, width), BF16),
            vmem((5, columns, spare, width), BF16),
            dma((levels, 6)),
            dma((levels, 6)),
            dma((5, 2)),
            dma((4, 2)),
            dma((5, 2)),
            dma((4, 2)),
            dma((levels + 1, 6)),
            dma((levels + 1, 6)),
            dma((4, 2)),
            dma((5, 2)),
            dma((4, 2)),
            dma((5, 2)),
            dma((chips - 1,)),
            dma((chips - 1,)),
            dma((3,)),
            dma((3,)),
            pltpu.SemaphoreType.REGULAR((4,)),
            dma((6,)),
        ],
        compiler_params=pltpu.CompilerParams(
            collective_id=0, has_side_effects=True, vmem_limit_bytes=53 * 2**20
        ),
        name="layer",
    )(tokens, stay(expert_ids.T), stay(route_weights.T), w_gate, w_up, w_down)


def expert_ffn(rows, gate_proj, up_proj, down_proj):
    gate = jnp.dot(rows, gate_proj, preferred_element_type=jnp.float32)
    upper = jnp.dot(rows, up_proj, preferred_element_type=jnp.float32)
    hidden = (jax.nn.silu(gate) * upper).astype(jnp.bfloat16)
    return jnp.dot(hidden, down_proj, preferred_element_type=jnp.float32).astype(jnp.bfloat16)


def on_device(tokens, expert_ids, route_weights, w_gate, w_up, w_down):
    tok_rows = tokens.shape[0]
    width = tokens.shape[1]
    top_count = expert_ids.shape[1]
    side_count = lax.axis_size("side")
    device_count = side_count * lax.axis_size("lane")
    local_count = w_gate.shape[0]
    expert_count = device_count * local_count
    capacity = 2 * tok_rows * top_count // expert_count
    flat_ids = expert_ids.reshape(-1)
    onehot = (flat_ids[:, None] == jnp.arange(expert_count, dtype=jnp.int32)[None, :]).astype(
        jnp.int32
    )
    earlier = jnp.cumsum(onehot, axis=0) - onehot
    slot_index = jnp.sum(earlier * onehot, axis=1)
    position = (flat_ids * capacity + slot_index).reshape(tok_rows, top_count)
    buffer_rows = jnp.arange(expert_count * capacity, dtype=jnp.int32)
    dispatch_table = jnp.any(buffer_rows[:, None, None] == position[None, :, :], axis=2).astype(
        jnp.bfloat16
    )
    outgoing = jnp.dot(dispatch_table, tokens, preferred_element_type=jnp.float32).astype(
        jnp.bfloat16
    )
    outgoing = outgoing.reshape(expert_count, capacity, width)
    received = lax.all_to_all(outgoing, ("side", "lane"), split_axis=0, concat_axis=0, tiled=True)
    count = received.shape[1]
    grouped = received.reshape(device_count, local_count, count, width)
    rows = grouped[:, 0].reshape(device_count * count, width)
    output = expert_ffn(rows, w_gate[0], w_up[0], w_down[0])
    results = [output.reshape(device_count, count, width)]
    returned = lax.all_to_all(
        jnp.stack(results, axis=1).reshape(device_count * local_count, count, width),
        ("side", "lane"),
        split_axis=0,
        concat_axis=0,
        tiled=True,
    )
    flat_back = returned.reshape(expert_count * capacity, width)
    picked = flat_back[position]
    mixed = jnp.einsum("tk,tkd->td", route_weights, picked, preferred_element_type=jnp.float32)
    return mixed.astype(jnp.bfloat16)


def layered(mesh, tokens):
    side, levels = mesh.shape["side"], mesh.shape["lane"]
    layer_bytes = tokens.shape[0] // 2 * tokens.shape[1] * tokens.dtype.itemsize
    fits = 3 * layer_bytes < 32 * 2**20 and side * levels <= tokens.shape[0] // (side * levels) == 2**7
    return side == 2**3 and levels == 4 and fits


def solution(mesh):
    placed = (
        P(AXES, None),
        P(AXES, None),
        P(AXES, None),
        P(AXES, None, None),
        P(AXES, None, None),
        P(AXES, None, None),
    )

    def run(tokens, *rest):
        body = on_device
        if layered(mesh, tokens):
            body = functools.partial(on_layers, mesh.shape["lane"])
        return jax.shard_map(
            body, mesh=mesh, in_specs=placed, out_specs=P(AXES, None), check_vma=False
        )(tokens, *rest)

    return run
```
